32 devices in a mesh: feat: 8 (over z, y), samp: 4 (over x, core).
Axes of the slice: x: 2, y: 2, z: 4, core: 2. Of those that a mesh axis runs over, the one named last changes fastest.
Arguments:
- design: bfloat16 [14336, 8192], P('samp', 'feat'), may hold values from -0.0625 to 0.0625
- targets: bfloat16 [14336, 128], P('samp'), may hold values from -26 to 26
- warm_start: float32 [8192, 128], P('feat'), may hold values from -0.6 to 0.6
- active_mask: int32 [2, 8192], P(None, 'feat'), may hold values 0 or 1
- penalty_index: int32 [1], replicated, may hold values from 0 to 7
Outputs:
- coefficients: float32 [8192, 128], P('feat')
- correlations: float32 [3, 8192], P(None, 'feat')
- relative_gaps: float32 [3], replicated
- pruned_counts: float32 [2], replicated
The draws below stay inside these ranges and needn't reach their ends.
All inputs are finite; a program needn't handle non-finite values. No bound on the sum of `active_mask` on one device may be relied on, other than what follows from the above.
Results may differ from the reference program's by a relative error of at most 0.0024.
The reference program's roundings to bfloat16 on the way count: a program that leaves them out, or rounds other values in their place, can miss the bound.
Values may be sent and summed in bfloat16 or wider, within the bound.
A program may use at most 64 MiB of HBM per device.

```python
import jax
import jax.numpy as jnp
from jax import lax

K = 128
ITERS = 2
NS = 14336
P_SIZE = 8192


def draw_targets(key, part):
    phase_key = jax.random.fold_in(key, 11)
    rough_key = jax.random.fold_in(key, 12)
    noise_key = jax.random.fold_in(key, 13)
    positions = jnp.arange(NS).astype(jnp.float32) / NS
    phase = jax.random.uniform(phase_key, (), jnp.float32, 0.0, 6.2831853)
    profile = jnp.exp(1.5 * jnp.sin(6.2831853 * 3.0 * positions + phase))
    rough = jax.random.uniform(rough_key, (NS, 1), jnp.float32, 0.7, 1.4)
    noise = jnp.clip(jax.random.normal(noise_key, (NS, K), jnp.float32), -4.0, 4.0)
    return (noise * profile[:, None] * rough).astype(jnp.bfloat16)


def plant(drawn, key, smallest, top_value):
    extent = drawn.shape
    index_at = [jax.random.randint(jax.random.fold_in(key, axis), (), 0, extent[axis]) for axis in range(len(extent))]
    drawn = drawn.at[tuple(index_at)].set(smallest)
    longest = extent.index(max(extent))
    index_at[longest] = (index_at[longest] + 1) % extent[longest]
    return drawn.at[tuple(index_at)].set(top_value)


def with_spikes(values, own_key, source, target, parts, factor):
    owner, partner = [(jnp.arange(values.shape[axis_at]) // (values.shape[axis_at] // parts)).reshape([-1 if axis == axis_at else 1 for axis in range(values.ndim)]) for axis_at in (source, target)]
    chosen = jax.random.permutation(own_key, parts)[partner]
    strong = (owner == chosen) | (owner == (partner + parts // 2) % parts)
    return jnp.where(strong, factor * values, values)


def levels(rng, extent, pieces, least, high):
    loudness, own = 1.0, jax.random.fold_in(rng, 6)
    for dim, blocks in pieces:
        steps = jnp.exp(jax.random.uniform(jax.random.fold_in(own, dim), (blocks,), jnp.float32, least / len(pieces), high / len(pieces)))
        loudness = loudness * jnp.repeat(steps, extent[dim] // blocks).reshape([-1 if axis == dim else 1 for axis in range(len(extent))])
    return loudness


def scatter_about(stream_key, extent, scale, reach, cuts=(), held_as=jnp.bfloat16):
    drawn = jax.random.normal(stream_key, extent, jnp.float32) * scale
    if len(cuts) > 0:
        drawn = levels(stream_key, extent, cuts, -0.22, 0.18) * drawn
    return jnp.clip(drawn, min=-reach, max=reach).astype(held_as)


def gaussian_with(stream_key, shape, spread, bound, shards, heavy, kind=jnp.bfloat16):
    result = spread * jax.random.normal(stream_key, shape, jnp.float32)
    if shards:
        result = result * levels(stream_key, shape, shards, -0.22, 0.18)
    return jnp.clip(with_spikes(result, jax.random.fold_in(stream_key, 3), *heavy), -bound, bound).astype(kind)


def setup_inputs(seed: int = 0) -> dict:
    key_list = jax.random.split(jax.random.key(seed), 6)
    design = gaussian_with(key_list[0], (NS, P_SIZE), NS ** -0.5, 0.0625, ((0, 4), (1, 8)), (1, 0, 8, 2.0))
    targets = draw_targets(jax.random.fold_in(key_list[5], 71), 0)
    warm_start = scatter_about(key_list[2], (P_SIZE, K), 0.1, 0.6, ((0, 8),), jnp.float32)
    active_mask = plant((jax.random.randint(key_list[3], (ITERS, P_SIZE), 0, 4) < 3).astype(jnp.int32), jax.random.fold_in(key_list[3], 1), 0, 1)
    penalty_index = jax.random.randint(key_list[4], (1,), 0, 8).astype(jnp.int32)
    return {"design": design, "targets": targets, "warm_start": warm_start, "active_mask": active_mask, "penalty_index": penalty_index}


def group_norms(matrix):
    return jnp.sqrt(lax.optimization_barrier(jnp.sum(matrix * matrix, axis=1)))

def transpose_product(design, right_side):
    return lax.dot_general(design, right_side, (((0,), (0,)), ((), ())), preferred_element_type=jnp.float32)

def reference(design, targets, warm_start, active_mask, penalty_index):
    corr_y = transpose_product(design, targets)
    column_squares = lax.optimization_barrier(jnp.sum(jnp.square(design.astype(jnp.float32)), axis=0))
    penalty_max = jnp.max(group_norms(corr_y))
    penalty = penalty_max / (8.0 + 4.0 * penalty_index[0].astype(jnp.float32))
    step_sizes = 0.5 / (1.0 + column_squares)
    target_float = targets.astype(jnp.float32)
    current = warm_start
    correlations = []
    relative_gaps = []
    pruned_counts = []
    for iteration in range(ITERS + 1):
        current_half = current.astype(jnp.bfloat16)
        fitted = jnp.dot(design, current_half, preferred_element_type=jnp.float32)
        residual = (target_float - fitted).astype(jnp.bfloat16)
        resid_float = residual.astype(jnp.float32)
        rr_sum = jnp.sum(resid_float * resid_float)
        ry_sum = jnp.sum(resid_float * target_float)
        bn_sum = jnp.sum(group_norms(current))
        gradient = transpose_product(design, residual)
        grad_norms = group_norms(gradient)
        scale = jnp.maximum(penalty, jnp.max(grad_norms))
        correlations.append(grad_norms / scale)
        primal = 0.5 * rr_sum + penalty * bn_sum
        ratio = penalty / scale
        dual = ratio * ry_sum - 0.5 * ratio * ratio * rr_sum
        relative_gaps.append((primal - dual) / (primal + 1.0))
        if iteration < ITERS:
            keep = active_mask[iteration].astype(jnp.float32)
            pruned_counts.append(jnp.sum(1.0 - keep))
            moved = current + step_sizes[:, None] * gradient
            moved_norms = group_norms(moved)
            cutoff = step_sizes * penalty
            factor = jnp.maximum(moved_norms - cutoff, 0.0) / jnp.maximum(moved_norms, cutoff)
            current = (keep * factor)[:, None] * moved
    return (current, jnp.stack(correlations), jnp.stack(relative_gaps), jnp.stack(pruned_counts))
```

```python
import functools

import jax
import jax.numpy as jnp
from jax import lax
from jax.experimental import pallas as pl
from jax.experimental.pallas import tpu as pltpu
from jax.sharding import PartitionSpec as P

ITERS = 2
F32 = jnp.float32
BF16 = jnp.bfloat16
LANES = 128
GROUP = 256
PER = 2
LINE = 4
CORES = 2
STATS = 16
MESH = pl.DeviceIdType.MESH


def fold(row, combine):
    pieces = [row[:, at : at + LANES] for at in range(0, row.shape[1], LANES)]
    return functools.reduce(combine, pieces)


def column_norms(matrix):
    return jnp.sqrt(jnp.sum(matrix * matrix, axis=0, keepdims=True))


def kernel(
    stored, stored_targets, stored_warm, mask, index, coef_out, corr_out, info_out,
    design, targets, warm, half, cur, ysend, yrecv, zsend, frecv, erecv, resid, mine, turned,
    gacc, cacc, drecv, dcrecv, gsend, grecv, sqs, sqr, coefs, nrm, mx, sums, exf, exs,
    l_s, t_s, w_s, y_s, y_r, z_s, f_r, e_r, b_s, a_s, a_r, d_s, d_r, x_s, x_r, h_s, h_r, q_s, q_r,
    c_s, c_r, n_s, n_r, m_s, m_r, ef_s, ef_r, es_s, es_r,
):
    T = ITERS + 1
    F = exf.shape[0]
    S = exs.shape[0]
    R, C = design.shape
    K = targets.shape[1]
    H = R // 2
    G = H // GROUP
    b = GROUP // PER
    pieces = CORES * 2
    W = C // pieces
    f = lax.axis_index("feat")
    s = lax.axis_index("samp")
    z, y = f // 2, lax.rem(f, 2)
    x, c = s // CORES, lax.rem(s, CORES)
    mid = lax.rem((z + 1) // 2, 2)
    is_mid = mid == 1
    is_end = mid == 0
    me = f * CORES + c
    near = z + 1 - 2 * lax.rem(z, 2)
    across = {"feat": z * 2 + 1 - y}
    nearby = {"feat": near * 2 + y}
    middle = {"feat": (LINE - 1 - z) * 2 + y}
    sibling = {"samp": x * CORES + 1 - c}
    facing = {"samp": (1 - x) * CORES + c}

    def remote(src, dst, send, recv, to):
        return pltpu.make_async_remote_copy(
            src_ref=src, dst_ref=dst, send_sem=send, recv_sem=recv, device_id=to, device_id_type=MESH
        )

    def peer(off):
        to = lax.rem(me + off, F * CORES)
        return {"feat": to // CORES, "samp": x * CORES + lax.rem(to, CORES)}

    def rows_at(side, g):
        return pl.ds(pl.multiple_of(side * H + g * GROUP, GROUP), GROUP)

    def load(side, g):
        at = rows_at(side, g)
        return pltpu.make_async_copy(stored.at[at, :], design.at[at, :], l_s.at[side, g])

    load_targets = pltpu.make_async_copy(stored_targets, targets, t_s)
    load_warm = pltpu.make_async_copy(stored_warm, warm, w_s)

    def copy_y(t, k):
        at = (t, k)
        return remote(ysend.at[at], yrecv.at[at], y_s.at[at], y_r.at[at], across)

    def copy_fold(t, k):
        at = (t, k)
        return remote(zsend.at[at], frecv.at[at], z_s.at[at], f_r.at[at], nearby)

    def copy_middle(t, k):
        at = (t, k)
        return remote(zsend.at[at], erecv.at[at], z_s.at[at], e_r.at[at], middle)

    def copy_out(t, k):
        ref = resid.at[t, y, k]
        return remote(ref, ref, b_s.at[t, k], f_r.at[t, k], nearby)

    def copy_a(t, k):
        ref = resid.at[t, y, k]
        return remote(ref, ref, a_s.at[t, k], a_r.at[t, k], across)

    def copy_d(t, j):
        at = (t, j)
        if t == T:
            return remote(cacc.at[(1 - c) * 2 + j], dcrecv.at[j], d_s.at[at], d_r.at[at], sibling)
        return remote(gacc.at[t, (1 - c) * 2 + j], drecv.at[at], d_s.at[at], d_r.at[at], sibling)

    def copy_x(t, j):
        at = (t, j)
        return remote(gsend.at[at], grecv.at[at], x_s.at[at], x_r.at[at], facing)

    def copy_h(t, j):
        ref = half.at[t, c * 2 + j]
        return remote(ref, ref, h_s.at[t, j], h_r.at[t, j], sibling)

    def copy_q(j):
        return remote(sqs.at[j], sqr.at[j], q_s.at[j], q_r.at[j], facing)

    def copy_c(j):
        ref = coefs.at[c * 2 + j]
        return remote(ref, ref, c_s.at[j], c_r.at[j], sibling)

    def copy_n():
        return remote(nrm.at[c], nrm.at[c], n_s, n_r, sibling)

    def copy_m(t, off):
        ref = mx.at[t, me]
        return remote(ref, ref, m_s.at[t, off], m_r.at[t, off], peer(off))

    def copy_ef(off):
        to = {"feat": lax.rem(f + off, F)}
        return remote(exf.at[f], exf.at[f], ef_s.at[off], ef_r.at[off], to)

    def copy_es(off):
        to = {"samp": lax.rem(s + off, S)}
        return remote(exs.at[s], exs.at[s], es_s.at[off], es_r.at[off], to)

    def each(first, count, body):
        def step(at, carry):
            body(at)
            return carry

        lax.fori_loop(first, count, step, 0)

    barrier = pltpu.get_barrier_semaphore()
    for off in range(1, F * CORES):
        pl.semaphore_signal(barrier, inc=1, device_id=peer(off), device_id_type=MESH)
    for core in range(CORES):
        to = {"samp": (1 - x) * CORES + core}
        pl.semaphore_signal(barrier, inc=1, device_id=to, device_id_type=MESH)
    load_warm.start()
    each(0, G, lambda g: load(1 - y, g).start())
    each(0, G, lambda g: load(y, g).start())
    load_targets.start()

    def share(t, side, g):
        return jnp.dot(design[rows_at(side, g), :], half[t].reshape(C, K), preferred_element_type=F32)

    def products(acc, rows, chunk, order):
        turned[...] = chunk.T
        for p in order:
            cols = pl.ds(pl.multiple_of(p * W, W), W)
            piece = jnp.dot(turned[...], design[rows, cols], preferred_element_type=F32)
            acc[p, 0:K] = acc[p, 0:K] + piece

    def grad_group(t, side, g, order=tuple(range(pieces))):
        chunk = resid[t, side, pl.ds(g * PER, PER)].reshape(GROUP, K)
        products(gacc.at[t], rows_at(side, g), chunk, order)

    def corr_group(at):
        rows = pl.ds(pl.multiple_of(at * GROUP, GROUP), GROUP)
        products(cacc, rows, targets[rows, :], range(pieces))
        tall = 16

        def body(i, acc):
            block = design[pl.ds(pl.multiple_of(at * GROUP + i * tall, tall), tall), :].astype(F32)
            block = block * block
            return acc + block[:8] + block[8:]

        acc = lax.fori_loop(0, GROUP // tall, body, jnp.zeros((8, C), F32), unroll=4)
        for p in range(pieces):
            cacc[p, K : K + 8] = cacc[p, K : K + 8] + acc[:, p * W : (p + 1) * W]

    def send_group(t, g):
        if t == 0:
            load(1 - y, g).wait()
        part = share(t, 1 - y, g).astype(BF16).reshape(PER, b, K)
        for j in range(PER):
            ysend[t, g * PER + j] = part[j]
        if t == 0:
            @pl.when(g == 0)
            def _():
                pl.semaphore_wait(barrier, F * CORES + CORES - 1)
        for j in range(PER):
            copy_y(t, g * PER + j).start()

    def fold_group(t, g):
        mine[...] = share(t, y, g)
        for j in range(PER):
            k = g * PER + j
            own = mine[j * b : (j + 1) * b]
            copy_y(t, k).wait_recv()

            @pl.when(is_end)
            def _():
                zsend[t, k] = (own + yrecv[t, k].astype(F32)).astype(BF16)
                copy_fold(t, k).start()

            @pl.when(is_mid)
            def _():
                copy_fold(t, k).wait_recv()
                zsend[t, k] = (own + yrecv[t, k].astype(F32) + frecv[t, k].astype(F32)).astype(BF16)
                copy_middle(t, k).start()

    def resid_group(t, g):
        @pl.when(is_end)
        def _():
            for j in range(PER):
                copy_out(t, g * PER + j).wait_recv()
                copy_a(t, g * PER + j).start()

        @pl.when(is_mid)
        def _():
            rr = jnp.zeros((1, K), F32)
            ry = jnp.zeros((1, K), F32)
            for j in range(PER):
                k = g * PER + j
                at = pl.ds(pl.multiple_of(y * H + k * b, b), b)
                goal = targets[at, :].astype(F32)
                copy_middle(t, k).wait_recv()
                fitted = zsend[t, k].astype(F32) + erecv[t, k].astype(F32)
                rounded = (goal - fitted).astype(BF16)
                resid[t, y, k] = rounded
                copy_a(t, k).start()
                copy_out(t, k).start()
                wide = rounded.astype(F32)
                rr = rr + jnp.sum(wide * wide, axis=0, keepdims=True)
                ry = ry + jnp.sum(wide * goal, axis=0, keepdims=True)
            sums[t : t + 1] = sums[t : t + 1] + 0.5 * rr
            sums[T + t : T + t + 1] = sums[T + t : T + t + 1] + 0.5 * ry

        grad_group(t, y, g)

    def last_group(t, g):
        for j in range(PER):
            copy_a(t, g * PER + j).wait_recv()
        if isinstance(g, int):
            grad_group(t, 1 - y, g, ((1 - c) * 2, (1 - c) * 2 + 1))
            for j in range(2):
                copy_d(t, j).start()
            grad_group(t, 1 - y, g, (c * 2, c * 2 + 1))
        else:
            grad_group(t, 1 - y, g)

    lag_fold = 3 * mid
    lag_resid = G - 1 - mid
    lag_last = G + 1

    def run(t, first, count):
        def step(at):
            to_fold = at - lag_fold
            to_resid = at - lag_resid
            to_last = at - lag_last

            @pl.when((to_fold >= 0) & (to_fold < G))
            def _():
                fold_group(t, to_fold)

            @pl.when((to_resid >= 0) & (to_resid < G))
            def _():
                resid_group(t, to_resid)

            @pl.when(to_last >= 0)
            def _():
                last_group(t, to_last)

            if t == 0:
                @pl.when(at < G)
                def _():
                    corr_group(at * 2)
                    corr_group(at * 2 + 1)

        each(first, count, step)

    def chip_sum(t, j):
        p = c * 2 + j
        copy_d(t, j).wait_recv()
        if t == T:
            both = cacc[p] + dcrecv[j]
            sqs[j] = both[K : K + 8]
            copy_q(j).start()
            gsend[t, j] = both[:K].astype(BF16)
        else:
            gsend[t, j] = (gacc[t, p] + drecv[t, j]).astype(BF16)
        copy_x(t, j).start()

    def whole_sum(t, j):
        copy_x(t, j).wait_recv()
        return gsend[t, j].astype(F32) + grecv[t, j].astype(F32)

    def spread(t, rows):
        most = fold(jnp.concatenate(rows, axis=1), jnp.maximum)
        mx[t, me] = jnp.broadcast_to(most, (8, LANES))
        for off in range(1, F * CORES):
            copy_m(t, off).start()

    def highest(t):
        for off in range(1, F * CORES):
            copy_m(t, off).wait_recv()
        tile = functools.reduce(jnp.maximum, [mx[t, at] for at in range(F * CORES)])
        return jnp.max(tile[0:1], axis=1, keepdims=True)

    def add_row(at, row):
        sums[at : at + 1] = sums[at : at + 1] + 0.5 * row

    load_warm.wait()
    half[0] = warm[...].astype(BF16).reshape(pieces, W, K)
    each(0, G, lambda g: send_group(0, g))
    sums[...] = jnp.zeros_like(sums)
    cacc[...] = jnp.zeros_like(cacc)
    gacc[...] = jnp.zeros_like(gacc)
    for j in range(2):
        cur[j] = warm[pl.ds(pl.multiple_of((c * 2 + j) * W, W), W), :].T
        add_row(2 * T, fold(column_norms(cur[j]), jnp.add))
    nrm[c] = jnp.zeros((8, 2 * W), F32)
    load_targets.wait()
    each(0, G, lambda g: load(y, g).wait())

    penalty = None
    step_sizes = None
    for t in range(T):
        if t > 0:
            each(0, G, lambda g: send_group(t, g))
        if t == 0:
            run(0, 0, G)
            for j in range(2):
                copy_d(T, j).start()
            run(0, G, G + 2)
            for j in range(2):
                chip_sum(T, j)
            run(0, G + 2, G + 5)
            spread(T, [column_norms(whole_sum(T, j)) for j in range(2)])
            run(0, G + 5, 2 * G)
        elif t == ITERS:
            run(t, 0, 2 * G - 2)
            exf[f] = sums[...]
            for off in range(1, F):
                copy_ef(off).start()
            run(t, 2 * G - 2, 2 * G)
        else:
            run(t, 0, 2 * G)
        last_group(t, G - 1)
        if t == 0:
            penalty = highest(T) / (8.0 + 4.0 * index[0].astype(F32))
            step_sizes = []
            for j in range(2):
                copy_q(j).wait_recv()
                squares = jnp.sum(sqs[j] + sqr[j], axis=0, keepdims=True)
                step_sizes.append(0.5 / (1.0 + squares))
        for j in range(2):
            chip_sum(t, j)
        if t == ITERS:
            for off in range(1, F):
                copy_ef(off).wait_recv()
            exs[s] = functools.reduce(jnp.add, [exf[at] for at in range(F)])
            for off in range(1, S):
                copy_es(off).start()
        norms = []
        for j in range(2):
            gradient = whole_sum(t, j)
            norms.append(column_norms(gradient))
            if t < ITERS:
                at = pl.ds(pl.multiple_of((c * 2 + j) * W, W), W)
                keep = mask[t : t + 1, at].astype(F32)
                moved = cur[j] + step_sizes[j] * gradient
                moved_norms = column_norms(moved)
                cutoff = step_sizes[j] * penalty
                factor = jnp.maximum(moved_norms - cutoff, 0.0) / jnp.maximum(moved_norms, cutoff)
                after = (keep * factor) * moved
                cur[j] = after
                upright = after.T
                half[t + 1, c * 2 + j] = upright.astype(BF16)
                copy_h(t + 1, j).start()
                if t + 1 == ITERS:
                    coefs[c * 2 + j] = upright
                    copy_c(j).start()
                add_row(3 * T + t, fold(1.0 - keep, jnp.add))
                add_row(2 * T + t + 1, fold(column_norms(after), jnp.add))
            nrm[c, t : t + 1, j * W : (j + 1) * W] = norms[j]
        spread(t, norms)
        if t < ITERS:
            for j in range(2):
                copy_h(t + 1, j).wait_recv()

    copy_n().start()
    for j in range(2):
        copy_c(j).wait_recv()
    coef_out[...] = coefs[...].reshape(C, K)
    for off in range(1, S):
        copy_es(off).wait_recv()
    merged = functools.reduce(jnp.add, [exs[at] for at in range(S)])
    added_up = jnp.sum(merged, axis=1, keepdims=True)
    copy_n().wait_recv()
    lines = []
    for t in range(T):
        rr, ry, bn = (added_up[at : at + 1] for at in (t, T + t, 2 * T + t))
        scale = jnp.maximum(penalty, highest(t))
        primal = 0.5 * rr + penalty * bn
        ratio = penalty / scale
        dual = ratio * ry - 0.5 * ratio * ratio * rr
        lines.append((primal - dual) / (primal + 1.0))
        for core in range(CORES):
            corr_out[t : t + 1, core * 2 * W : (core + 1) * 2 * W] = nrm[core, t : t + 1, :] / scale
    for t in range(ITERS):
        lines.append(added_up[3 * T + t : 3 * T + t + 1])
    for at, line in enumerate(lines):
        info_out[at : at + 1, :] = jnp.broadcast_to(line, (1, LANES))

    for t in range(T):

        def drain(k):
            copy_y(t, k).wait_send()
            copy_fold(t, k).wait_send()
            copy_a(t, k).wait_send()

            @pl.when(is_mid)
            def _():
                copy_out(t, k).wait_send()

        each(0, G * PER, drain)
    for j in range(2):
        for t in range(T + 1):
            copy_d(t, j).wait_send()
            copy_x(t, j).wait_send()
        for t in range(1, T):
            copy_h(t, j).wait_send()
        copy_q(j).wait_send()
        copy_c(j).wait_send()
    copy_n().wait_send()
    for t in range(T + 1):
        for off in range(1, F * CORES):
            copy_m(t, off).wait_send()
    for off in range(1, F):
        copy_ef(off).wait_send()
    for off in range(1, S):
        copy_es(off).wait_send()


def finish(coef, corr, info, coef_out, corr_out, gaps_out, pruned_out):
    coef_out[...] = coef[...]
    corr_out[...] = corr[...]
    for at in range(ITERS + 1):
        gaps_out[at] = info[at, 0]
    for at in range(ITERS):
        pruned_out[at] = info[ITERS + 1 + at, 0]


def fused(design, targets, warm_start, active_mask, penalty_index):
    F, S = lax.axis_size("feat"), lax.axis_size("samp")
    R, C = design.shape
    K = targets.shape[1]
    T = ITERS + 1
    N = R // 2 // GROUP * PER
    b = GROUP // PER
    pieces = CORES * 2
    W = C // pieces
    dma = pltpu.SemaphoreType.DMA
    vmem = pl.BlockSpec(memory_space=pltpu.VMEM)
    anywhere = pl.BlockSpec(memory_space=pl.ANY)
    smem = pl.BlockSpec(memory_space=pltpu.SMEM)
    chunks = pltpu.VMEM((T, N, b, K), BF16)
    coefficients, correlations, info = pl.pallas_call(
        kernel,
        out_shape=(
            jax.ShapeDtypeStruct((C, K), F32),
            jax.ShapeDtypeStruct((T, C), F32),
            jax.ShapeDtypeStruct((8, LANES), F32),
        ),
        in_specs=[anywhere] * 3 + [vmem, smem],
        out_specs=(vmem,) * 3,
        scratch_shapes=[
            pltpu.VMEM((R, C), BF16),
            pltpu.VMEM((R, K), BF16),
            pltpu.VMEM((C, K), F32),
            pltpu.VMEM((T, pieces, W, K), BF16),
            pltpu.VMEM((2, K, W), F32),
            chunks,
            chunks,
            chunks,
            chunks,
            chunks,
            pltpu.VMEM((T, 2, N, b, K), BF16),
            pltpu.VMEM((GROUP, K), F32),
            pltpu.VMEM((K, GROUP), BF16),
            pltpu.VMEM((T, pieces, K, W), F32),
            pltpu.VMEM((pieces, K + 8, W), F32),
            pltpu.VMEM((T, 2, K, W), F32),
            pltpu.VMEM((2, K + 8, W), F32),
            pltpu.VMEM((T + 1, 2, K, W), BF16),
            pltpu.VMEM((T + 1, 2, K, W), BF16),
            pltpu.VMEM((2, 8, W), F32),
            pltpu.VMEM((2, 8, W), F32),
            pltpu.VMEM((pieces, W, K), F32),
            pltpu.VMEM((CORES, 8, 2 * W), F32),
            pltpu.VMEM((T + 1, F * CORES, 8, LANES), F32),
            pltpu.VMEM((STATS, LANES), F32),
            pltpu.VMEM((F, STATS, LANES), F32),
            pltpu.VMEM((S, STATS, LANES), F32),
        ]
        + [dma((2, N // PER)), dma, dma]
        + [dma((T, N))] * 8
        + [dma((T + 1, 2))] * 4
        + [dma((T, 2))] * 2
        + [dma((2,))] * 4
        + [dma, dma]
        + [dma((T + 1, F * CORES))] * 2
        + [dma((F,))] * 2
        + [dma((S,))] * 2,
        compiler_params=pltpu.CompilerParams(
            collective_id=0, has_side_effects=True, vmem_limit_bytes=62 * 1024 * 1024
        ),
    )(design, targets, warm_start, active_mask, penalty_index)
    return pl.pallas_call(
        finish,
        out_shape=(
            jax.ShapeDtypeStruct((C, K), F32),
            jax.ShapeDtypeStruct((T, C), F32),
            jax.ShapeDtypeStruct((T,), F32),
            jax.ShapeDtypeStruct((ITERS,), F32),
        ),
        in_specs=[vmem, vmem, smem],
        out_specs=(vmem, vmem, smem, smem),
    )(coefficients, correlations, info)


def group_norms(matrix):
    return jnp.sqrt(jnp.sum(matrix * matrix, axis=1))


def transpose_product(design, right_side):
    return lax.dot_general(
        design, right_side, (((0,), (0,)), ((), ())), preferred_element_type=jnp.float32
    )


def plain(design, targets, warm_start, active_mask, penalty_index):
    row_count, col_count = design.shape
    feat_size = lax.axis_size("feat")
    feat_slot = lax.axis_index("feat")
    block_rows = row_count // feat_size
    samp_first = (lax.axis_index("samp") == 0).astype(jnp.float32)
    corr_local = transpose_product(design, targets)
    squares_local = jnp.sum(jnp.square(design.astype(jnp.float32)), axis=0)
    corr_y, column_squares = lax.psum((corr_local, squares_local), "samp")
    penalty_max = lax.pmax(jnp.max(group_norms(corr_y)), "feat")
    penalty = penalty_max / (8.0 + 4.0 * penalty_index[0].astype(jnp.float32))
    step_sizes = 0.5 / (1.0 + column_squares)
    current = warm_start
    correlations = []
    relative_gaps = []
    pruned_counts = []
    own_targets = lax.dynamic_slice_in_dim(targets, feat_slot * block_rows, block_rows, 0)
    for iteration in range(ITERS + 1):
        current_half = current.astype(jnp.bfloat16)
        fitted_part = jnp.dot(design, current_half, preferred_element_type=jnp.float32)
        fitted = lax.psum(fitted_part, "feat")
        residual_all = (targets.astype(jnp.float32) - fitted).astype(jnp.bfloat16)
        residual = lax.dynamic_slice_in_dim(residual_all, feat_slot * block_rows, block_rows, 0)
        grad_local = transpose_product(design, residual_all)
        resid_float = residual.astype(jnp.float32)
        rr_local = jnp.sum(resid_float * resid_float)
        ry_local = jnp.sum(resid_float * own_targets.astype(jnp.float32))
        bn_local = samp_first * jnp.sum(group_norms(current))
        if iteration < ITERS:
            keep = active_mask[iteration].astype(jnp.float32)
            pruned_local = samp_first * jnp.sum(1.0 - keep)
        else:
            pruned_local = jnp.zeros((), jnp.float32)
        gradient = lax.psum(grad_local, "samp")
        grad_norms = group_norms(gradient)
        local_max = jnp.max(grad_norms)
        grad_top = lax.pmax(local_max, "feat")
        rr_sum, ry_sum, bn_sum, pruned_sum = lax.psum(
            (rr_local, ry_local, bn_local, pruned_local), ("feat", "samp")
        )
        scale = jnp.maximum(penalty, grad_top)
        correlations.append(grad_norms / scale)
        primal = 0.5 * rr_sum + penalty * bn_sum
        ratio = penalty / scale
        dual = ratio * ry_sum - 0.5 * ratio * ratio * rr_sum
        relative_gaps.append((primal - dual) / (primal + 1.0))
        if iteration < ITERS:
            pruned_counts.append(pruned_sum)
            moved = current + step_sizes[:, None] * gradient
            moved_norms = group_norms(moved)
            cutoff = step_sizes * penalty
            factor = jnp.maximum(moved_norms - cutoff, 0.0) / jnp.maximum(moved_norms, cutoff)
            current = (keep * factor)[:, None] * moved
    return (current, jnp.stack(correlations), jnp.stack(relative_gaps), jnp.stack(pruned_counts))


def local(design, targets, warm_start, active_mask, penalty_index):
    feat, samp = lax.axis_size("feat"), lax.axis_size("samp")
    rows, cols = design.shape
    fits = (
        feat == 2 * LINE
        and samp == 2 * CORES
        and rows % (2 * GROUP) == 0
        and rows // (2 * GROUP) >= 6
        and cols % (2 * CORES * LANES) == 0
        and targets.shape[1] == LANES
    )
    form = fused if fits else plain
    return form(design, targets, warm_start, active_mask, penalty_index)


def solution(mesh):
    placed = (P("samp", "feat"), P("samp", None), P("feat", None), P(None, "feat"), P())
    return jax.shard_map(
        local,
        mesh=mesh,
        in_specs=placed,
        out_specs=(P("feat", None), P(None, "feat"), P(), P()),
        check_vma=False,
    )
```

```python
import functools

import jax
import jax.numpy as jnp
from jax import lax
from jax.experimental import pallas as pl
from jax.experimental.pallas import tpu as pltpu
from jax.sharding import PartitionSpec as P

ITERS = 2
F32 = jnp.float32
BF16 = jnp.bfloat16
LANES = 128
GROUP = 256
PER = 2
LINE = 4
CORES = 2
STATS = 16
MESH = pl.DeviceIdType.MESH


def fold(row, combine):
    pieces = [row[:, at : at + LANES] for at in range(0, row.shape[1], LANES)]
    return functools.reduce(combine, pieces)


def column_norms(matrix):
    return jnp.sqrt(jnp.sum(matrix * matrix, axis=0, keepdims=True))


def kernel(
    stored, stored_targets, stored_warm, mask, index, coef_out, corr_out, info_out,
    design, targets, warm, half, cur, ysend, yrecv, zsend, frecv, erecv, resid, mine, turned,
    gacc, cacc, drecv, dcrecv, gsend, grecv, sqs, sqr, coefs, nrm, mx, sums, exf, exs,
    l_s, o_s, t_s, w_s, y_s, z_s, b_s, a_s, d_s, dc_s, x_s, h_s, q_s, c_s, n_s, m_s, ef_s, es_s,
    y_r, f_r, e_r, a_r, d_r, dc_r, h_r, x_r, m_r, q_r, c_r, n_r, ef_r, es_r,
):
    T = ITERS + 1
    F = exf.shape[0]
    S = exs.shape[0]
    R, C = design.shape
    K = targets.shape[1]
    H = R // 2
    G = H // GROUP
    b = GROUP // PER
    pieces = CORES * 2
    W = C // pieces
    f = lax.axis_index("feat")
    s = lax.axis_index("samp")
    z, y = f // 2, lax.rem(f, 2)
    x, c = s // CORES, lax.rem(s, CORES)
    mid = lax.rem((z + 1) // 2, 2)
    is_mid = mid == 1
    is_end = mid == 0
    me = f * CORES + c
    near = z + 1 - 2 * lax.rem(z, 2)
    across = {"feat": z * 2 + 1 - y}
    nearby = {"feat": near * 2 + y}
    middle = {"feat": (LINE - 1 - z) * 2 + y}
    sibling = {"samp": x * CORES + 1 - c}
    facing = {"samp": (1 - x) * CORES + c}

    def remote(src, dst, send, recv, to):
        return pltpu.make_async_remote_copy(
            src_ref=src, dst_ref=dst, send_sem=send, recv_sem=recv, device_id=to, device_id_type=MESH
        )

    def peer(off):
        to = lax.rem(me + off, F * CORES)
        return {"feat": to // CORES, "samp": x * CORES + lax.rem(to, CORES)}

    def rows_at(side, g):
        return pl.ds(pl.multiple_of(side * H + g * GROUP, GROUP), GROUP)

    def load(g):
        at = rows_at(1 - y, g)
        return pltpu.make_async_copy(stored.at[at, :], design.at[at, :], l_s.at[g])

    own_rows = pl.ds(pl.multiple_of(y * H, H), H)
    load_own = pltpu.make_async_copy(stored.at[own_rows, :], design.at[own_rows, :], o_s)

    load_targets = pltpu.make_async_copy(stored_targets, targets, t_s)
    load_warm = pltpu.make_async_copy(stored_warm, warm, w_s)

    def copy_y(t, k):
        at = (t, k)
        return remote(ysend.at[at], yrecv.at[at], y_s, y_r.at[k], across)

    def copy_fold(t, k):
        at = (t, k)
        return remote(zsend.at[at], frecv.at[at], z_s, f_r.at[k], nearby)

    def copy_middle(t, k):
        at = (t, k)
        return remote(zsend.at[at], erecv.at[at], z_s, e_r.at[k], middle)

    def copy_out(t, k):
        ref = resid.at[t, y, k]
        return remote(ref, ref, b_s, f_r.at[k], nearby)

    def copy_a(t, k):
        ref = resid.at[t, y, k]
        return remote(ref, ref, a_s, a_r.at[k], across)

    def copy_d(t, j):
        at = (t, j)
        if t == T:
            return remote(cacc.at[(1 - c) * 2 + j], dcrecv.at[j], dc_s, dc_r.at[j], sibling)
        return remote(gacc.at[t, (1 - c) * 2 + j], drecv.at[at], d_s, d_r.at[j], sibling)

    def copy_x(t, j):
        at = (t, j)
        return remote(gsend.at[at], grecv.at[at], x_s, x_r.at[at], facing)

    def copy_h(t, j):
        ref = half.at[t, c * 2 + j]
        return remote(ref, ref, h_s, h_r.at[j], sibling)

    def copy_q():
        return remote(sqs, sqr, q_s, q_r, facing)

    def copy_c():
        ref = coefs.at[pl.ds(c * 2, 2)]
        return remote(ref, ref, c_s, c_r, sibling)

    def copy_n():
        return remote(nrm.at[c], nrm.at[c], n_s, n_r, sibling)

    def copy_m(t, off):
        ref = mx.at[t, me]
        return remote(ref, ref, m_s, m_r.at[t], peer(off))

    def copy_ef(off):
        to = {"feat": lax.rem(f + off, F)}
        return remote(exf.at[f], exf.at[f], ef_s, ef_r, to)

    def copy_es(off):
        to = {"samp": lax.rem(s + off, S)}
        return remote(exs.at[s], exs.at[s], es_s, es_r, to)

    others_f = exf.at[pl.ds(0, F - 1)]
    others_s = exs.at[pl.ds(0, S - 1)]

    def each(first, count, body):
        def step(at, carry):
            body(at)
            return carry

        lax.fori_loop(first, count, step, 0)

    barrier = pltpu.get_barrier_semaphore()
    for off in range(1, F * CORES):
        pl.semaphore_signal(barrier, inc=1, device_id=peer(off), device_id_type=MESH)
    for core in range(CORES):
        to = {"samp": (1 - x) * CORES + core}
        pl.semaphore_signal(barrier, inc=1, device_id=to, device_id_type=MESH)
    load_warm.start()
    each(0, G, lambda g: load(g).start())
    load_own.start()
    load_targets.start()

    def share(t, side, g):
        return jnp.dot(design[rows_at(side, g), :], half[t].reshape(C, K), preferred_element_type=F32)

    def products(acc, rows, chunk, order):
        turned[...] = chunk.T
        for p in order:
            cols = pl.ds(pl.multiple_of(p * W, W), W)
            piece = jnp.dot(turned[...], design[rows, cols], preferred_element_type=F32)
            acc[p, 0:K] = acc[p, 0:K] + piece

    def grad_group(t, side, g, order=tuple(range(pieces))):
        chunk = resid[t, side, pl.ds(g * PER, PER)].reshape(GROUP, K)
        products(gacc.at[t], rows_at(side, g), chunk, order)

    def corr_group(at):
        rows = pl.ds(pl.multiple_of(at * GROUP, GROUP), GROUP)
        products(cacc, rows, targets[rows, :], range(pieces))
        tall = 16

        def body(i, acc):
            block = design[pl.ds(pl.multiple_of(at * GROUP + i * tall, tall), tall), :].astype(F32)
            block = block * block
            return acc + block[:8] + block[8:]

        acc = lax.fori_loop(0, GROUP // tall, body, jnp.zeros((8, C), F32), unroll=4)
        for p in range(pieces):
            cacc[p, K : K + 8] = cacc[p, K : K + 8] + acc[:, p * W : (p + 1) * W]

    def send_group(t, g, ready=True):
        if t == 0:
            load(g).wait()
        part = share(t, 1 - y, g).astype(BF16).reshape(PER, b, K)
        for j in range(PER):
            ysend[t, g * PER + j] = part[j]
        if not ready:
            pl.semaphore_wait(barrier, F * CORES + CORES - 1)
        for j in range(PER):
            copy_y(t, g * PER + j).start()

    def fold_group(t, g):
        mine[...] = share(t, y, g)
        for j in range(PER):
            k = g * PER + j
            own = mine[j * b : (j + 1) * b]
            copy_y(t, k).wait_recv()

            @pl.when(is_end)
            def _():
                zsend[t, k] = (own + yrecv[t, k].astype(F32)).astype(BF16)
                copy_fold(t, k).start()

            @pl.when(is_mid)
            def _():
                copy_fold(t, k).wait_recv()
                zsend[t, k] = (own + yrecv[t, k].astype(F32) + frecv[t, k].astype(F32)).astype(BF16)
                copy_middle(t, k).start()

    def resid_group(t, g):
        @pl.when(is_end)
        def _():
            for j in range(PER):
                copy_out(t, g * PER + j).wait_recv()
                copy_a(t, g * PER + j).start()

        @pl.when(is_mid)
        def _():
            rr = jnp.zeros((1, K), F32)
            ry = jnp.zeros((1, K), F32)
            for j in range(PER):
                k = g * PER + j
                at = pl.ds(pl.multiple_of(y * H + k * b, b), b)
                goal = targets[at, :].astype(F32)
                copy_middle(t, k).wait_recv()
                fitted = zsend[t, k].astype(F32) + erecv[t, k].astype(F32)
                rounded = (goal - fitted).astype(BF16)
                resid[t, y, k] = rounded
                copy_a(t, k).start()
                copy_out(t, k).start()
                wide = rounded.astype(F32)
                rr = rr + jnp.sum(wide * wide, axis=0, keepdims=True)
                ry = ry + jnp.sum(wide * goal, axis=0, keepdims=True)
            sums[t : t + 1] = sums[t : t + 1] + 0.5 * rr
            sums[T + t : T + t + 1] = sums[T + t : T + t + 1] + 0.5 * ry

        grad_group(t, y, g)

    def last_group(t, g):
        for j in range(PER):
            copy_a(t, g * PER + j).wait_recv()
        if isinstance(g, int):
            grad_group(t, 1 - y, g, ((1 - c) * 2, (1 - c) * 2 + 1))
            for j in range(2):
                copy_d(t, j).start()
            grad_group(t, 1 - y, g, (c * 2, c * 2 + 1))
        else:
            grad_group(t, 1 - y, g)

    lag_fold = 3 * mid
    lag_resid = G - 1 - mid
    lag_last = G + 1

    def run(t, first, count):
        def step(at):
            to_fold = at - lag_fold
            to_resid = at - lag_resid
            to_last = at - lag_last

            @pl.when((to_fold >= 0) & (to_fold < G))
            def _():
                fold_group(t, to_fold)

            @pl.when((to_resid >= 0) & (to_resid < G))
            def _():
                resid_group(t, to_resid)

            @pl.when(to_last >= 0)
            def _():
                last_group(t, to_last)

            if t == 0:
                @pl.when(at < G)
                def _():
                    corr_group(at * 2)
                    corr_group(at * 2 + 1)

        each(first, count, step)

    def chip_sum(t, j):
        p = c * 2 + j
        copy_d(t, j).wait_recv()
        if t == T:
            both = cacc[p] + dcrecv[j]
            sqs[j] = both[K : K + 8]
            gsend[t, j] = both[:K].astype(BF16)
        else:
            gsend[t, j] = (gacc[t, p] + drecv[t, j]).astype(BF16)
        copy_x(t, j).start()

    def whole_sum(t, j):
        copy_x(t, j).wait_recv()
        return gsend[t, j].astype(F32) + grecv[t, j].astype(F32)

    def spread(t, rows):
        most = fold(jnp.concatenate(rows, axis=1), jnp.maximum)
        mx[t, me] = jnp.broadcast_to(most, (8, LANES))
        for off in range(1, F * CORES):
            copy_m(t, off).start()

    def highest(t):
        several = mx.at[t, pl.ds(0, F * CORES - 1)]
        remote(several, several, m_s, m_r.at[t], peer(1)).wait_recv()
        tile = functools.reduce(jnp.maximum, [mx[t, at] for at in range(F * CORES)])
        return jnp.max(tile[0:1], axis=1, keepdims=True)

    def add_row(at, row):
        sums[at : at + 1] = sums[at : at + 1] + 0.5 * row

    load_warm.wait()
    half[0] = warm[...].astype(BF16).reshape(pieces, W, K)
    send_group(0, 0, False)
    each(1, G, lambda g: send_group(0, g))
    sums[...] = jnp.zeros_like(sums)
    cacc[...] = jnp.zeros_like(cacc)
    gacc[...] = jnp.zeros_like(gacc)
    for j in range(2):
        cur[j] = warm[pl.ds(pl.multiple_of((c * 2 + j) * W, W), W), :].T
        add_row(2 * T, fold(column_norms(cur[j]), jnp.add))
    nrm[c] = jnp.zeros((8, 2 * W), F32)
    load_targets.wait()
    load_own.wait()

    penalty = None
    step_sizes = None
    for t in range(T):
        if t > 0:
            each(0, G, lambda g: send_group(t, g))
        if t == 0:
            run(0, 0, G)
            for j in range(2):
                copy_d(T, j).start()
            run(0, G, G + 2)
            for j in range(2):
                chip_sum(T, j)
            copy_q().start()
            run(0, G + 2, G + 5)
            spread(T, [column_norms(whole_sum(T, j)) for j in range(2)])
            run(0, G + 5, 2 * G)
        elif t == ITERS:
            run(t, 0, 2 * G - 2)
            exf[f] = sums[...]
            for off in range(1, F):
                copy_ef(off).start()
            run(t, 2 * G - 2, 2 * G)
        else:
            run(t, 0, 2 * G)
        last_group(t, G - 1)
        if t == 0:
            penalty = highest(T) / (8.0 + 4.0 * index[0].astype(F32))
            step_sizes = []
            copy_q().wait_recv()
            for j in range(2):
                squares = jnp.sum(sqs[j] + sqr[j], axis=0, keepdims=True)
                step_sizes.append(0.5 / (1.0 + squares))
        for j in range(2):
            chip_sum(t, j)
        if t == ITERS:
            remote(others_f, others_f, ef_s, ef_r, across).wait_recv()
            exs[s] = functools.reduce(jnp.add, [exf[at] for at in range(F)])
            for off in range(1, S):
                copy_es(off).start()
        norms = []
        for j in range(2):
            gradient = whole_sum(t, j)
            norms.append(column_norms(gradient))
            if t < ITERS:
                at = pl.ds(pl.multiple_of((c * 2 + j) * W, W), W)
                keep = mask[t : t + 1, at].astype(F32)
                moved = cur[j] + step_sizes[j] * gradient
                moved_norms = column_norms(moved)
                cutoff = step_sizes[j] * penalty
                factor = jnp.maximum(moved_norms - cutoff, 0.0) / jnp.maximum(moved_norms, cutoff)
                after = (keep * factor) * moved
                cur[j] = after
                upright = after.T
                half[t + 1, c * 2 + j] = upright.astype(BF16)
                copy_h(t + 1, j).start()
                if t + 1 == ITERS:
                    coefs[c * 2 + j] = upright
                add_row(3 * T + t, fold(1.0 - keep, jnp.add))
                add_row(2 * T + t + 1, fold(column_norms(after), jnp.add))
            nrm[c, t : t + 1, j * W : (j + 1) * W] = norms[j]
        spread(t, norms)
        if t + 1 == ITERS:
            copy_c().start()
        if t < ITERS:
            for j in range(2):
                copy_h(t + 1, j).wait_recv()

    copy_n().start()
    copy_c().wait_recv()
    coef_out[...] = coefs[...].reshape(C, K)
    remote(others_s, others_s, es_s, es_r, sibling).wait_recv()
    merged = functools.reduce(jnp.add, [exs[at] for at in range(S)])
    added_up = jnp.sum(merged, axis=1, keepdims=True)
    copy_n().wait_recv()
    lines = []
    for t in range(T):
        rr, ry, bn = (added_up[at : at + 1] for at in (t, T + t, 2 * T + t))
        scale = jnp.maximum(penalty, highest(t))
        primal = 0.5 * rr + penalty * bn
        ratio = penalty / scale
        dual = ratio * ry - 0.5 * ratio * ratio * rr
        lines.append((primal - dual) / (primal + 1.0))
        for core in range(CORES):
            corr_out[t : t + 1, core * 2 * W : (core + 1) * 2 * W] = nrm[core, t : t + 1, :] / scale
    for t in range(ITERS):
        lines.append(added_up[3 * T + t : 3 * T + t + 1])
    for at, line in enumerate(lines):
        info_out[at : at + 1, :] = jnp.broadcast_to(line, (1, LANES))

    def drain(ref, sem):
        remote(ref, ref, sem, n_r, sibling).wait_send()

    drain(ysend, y_s)
    drain(zsend, z_s)
    drain(ysend, a_s)

    @pl.when(is_mid)
    def _():
        drain(ysend, b_s)

    drain(gacc.at[:, pl.ds(0, 2)], d_s)
    drain(cacc.at[pl.ds(0, 2)], dc_s)
    drain(gsend, x_s)
    drain(half.at[pl.ds(0, ITERS), pl.ds(0, 2)], h_s)
    drain(sqs, q_s)
    drain(coefs.at[pl.ds(0, 2)], c_s)
    drain(nrm.at[0], n_s)
    drain(mx.at[:, pl.ds(0, F * CORES - 1)], m_s)
    drain(others_f, ef_s)
    drain(others_s, es_s)


def finish(coef, corr, info, coef_out, corr_out, gaps_out, pruned_out):
    coef_out[...] = coef[...]
    corr_out[...] = corr[...]
    for at in range(ITERS + 1):
        gaps_out[at] = info[at, 0]
    for at in range(ITERS):
        pruned_out[at] = info[ITERS + 1 + at, 0]


def fused(design, targets, warm_start, active_mask, penalty_index):
    F, S = lax.axis_size("feat"), lax.axis_size("samp")
    R, C = design.shape
    K = targets.shape[1]
    T = ITERS + 1
    N = R // 2 // GROUP * PER
    b = GROUP // PER
    pieces = CORES * 2
    W = C // pieces
    dma = pltpu.SemaphoreType.DMA
    vmem = pl.BlockSpec(memory_space=pltpu.VMEM)
    anywhere = pl.BlockSpec(memory_space=pl.ANY)
    smem = pl.BlockSpec(memory_space=pltpu.SMEM)
    chunks = pltpu.VMEM((T, N, b, K), BF16)
    coefficients, correlations, info = pl.pallas_call(
        kernel,
        out_shape=(
            jax.ShapeDtypeStruct((C, K), F32),
            jax.ShapeDtypeStruct((T, C), F32),
            jax.ShapeDtypeStruct((8, LANES), F32),
        ),
        in_specs=[anywhere] * 3 + [vmem, smem],
        out_specs=(vmem,) * 3,
        scratch_shapes=[
            pltpu.VMEM((R, C), BF16),
            pltpu.VMEM((R, K), BF16),
            pltpu.VMEM((C, K), F32),
            pltpu.VMEM((T, pieces, W, K), BF16),
            pltpu.VMEM((2, K, W), F32),
            chunks,
            chunks,
            chunks,
            chunks,
            chunks,
            pltpu.VMEM((T, 2, N, b, K), BF16),
            pltpu.VMEM((GROUP, K), F32),
            pltpu.VMEM((K, GROUP), BF16),
            pltpu.VMEM((T, pieces, K, W), F32),
            pltpu.VMEM((pieces, K + 8, W), F32),
            pltpu.VMEM((T, 2, K, W), F32),
            pltpu.VMEM((2, K + 8, W), F32),
            pltpu.VMEM((T + 1, 2, K, W), BF16),
            pltpu.VMEM((T + 1, 2, K, W), BF16),
            pltpu.VMEM((2, 8, W), F32),
            pltpu.VMEM((2, 8, W), F32),
            pltpu.VMEM((pieces, W, K), F32),
            pltpu.VMEM((CORES, 8, 2 * W), F32),
            pltpu.VMEM((T + 1, F * CORES, 8, LANES), F32),
            pltpu.VMEM((STATS, LANES), F32),
            pltpu.VMEM((F, STATS, LANES), F32),
            pltpu.VMEM((S, STATS, LANES), F32),
        ]
        + [dma((N // PER,))]
        + [dma] * 17
        + [dma((N,))] * 4
        + [dma((2,))] * 3
        + [dma((T + 1, 2)), dma((T + 1,))]
        + [dma] * 5,
        compiler_params=pltpu.CompilerParams(
            collective_id=0, has_side_effects=True, vmem_limit_bytes=62 * 1024 * 1024
        ),
    )(design, targets, warm_start, active_mask, penalty_index)
    return pl.pallas_call(
        finish,
        out_shape=(
            jax.ShapeDtypeStruct((C, K), F32),
            jax.ShapeDtypeStruct((T, C), F32),
            jax.ShapeDtypeStruct((T,), F32),
            jax.ShapeDtypeStruct((ITERS,), F32),
        ),
        in_specs=[vmem, vmem, smem],
        out_specs=(vmem, vmem, smem, smem),
    )(coefficients, correlations, info)


def group_norms(matrix):
    return jnp.sqrt(jnp.sum(matrix * matrix, axis=1))


def transpose_product(design, right_side):
    return lax.dot_general(
        design, right_side, (((0,), (0,)), ((), ())), preferred_element_type=jnp.float32
    )


def plain(design, targets, warm_start, active_mask, penalty_index):
    row_count, col_count = design.shape
    feat_size = lax.axis_size("feat")
    feat_slot = lax.axis_index("feat")
    block_rows = row_count // feat_size
    samp_first = (lax.axis_index("samp") == 0).astype(jnp.float32)
    corr_local = transpose_product(design, targets)
    squares_local = jnp.sum(jnp.square(design.astype(jnp.float32)), axis=0)
    corr_y, column_squares = lax.psum((corr_local, squares_local), "samp")
    penalty_max = lax.pmax(jnp.max(group_norms(corr_y)), "feat")
    penalty = penalty_max / (8.0 + 4.0 * penalty_index[0].astype(jnp.float32))
    step_sizes = 0.5 / (1.0 + column_squares)
    current = warm_start
    correlations = []
    relative_gaps = []
    pruned_counts = []
    own_targets = lax.dynamic_slice_in_dim(targets, feat_slot * block_rows, block_rows, 0)
    for iteration in range(ITERS + 1):
        current_half = current.astype(jnp.bfloat16)
        fitted_part = jnp.dot(design, current_half, preferred_element_type=jnp.float32)
        fitted = lax.psum(fitted_part, "feat")
        residual_all = (targets.astype(jnp.float32) - fitted).astype(jnp.bfloat16)
        residual = lax.dynamic_slice_in_dim(residual_all, feat_slot * block_rows, block_rows, 0)
        grad_local = transpose_product(design, residual_all)
        resid_float = residual.astype(jnp.float32)
        rr_local = jnp.sum(resid_float * resid_float)
        ry_local = jnp.sum(resid_float * own_targets.astype(jnp.float32))
        bn_local = samp_first * jnp.sum(group_norms(current))
        if iteration < ITERS:
            keep = active_mask[iteration].astype(jnp.float32)
            pruned_local = samp_first * jnp.sum(1.0 - keep)
        else:
            pruned_local = jnp.zeros((), jnp.float32)
        gradient = lax.psum(grad_local, "samp")
        grad_norms = group_norms(gradient)
        local_max = jnp.max(grad_norms)
        grad_top = lax.pmax(local_max, "feat")
        rr_sum, ry_sum, bn_sum, pruned_sum = lax.psum(
            (rr_local, ry_local, bn_local, pruned_local), ("feat", "samp")
        )
        scale = jnp.maximum(penalty, grad_top)
        correlations.append(grad_norms / scale)
        primal = 0.5 * rr_sum + penalty * bn_sum
        ratio = penalty / scale
        dual = ratio * ry_sum - 0.5 * ratio * ratio * rr_sum
        relative_gaps.append((primal - dual) / (primal + 1.0))
        if iteration < ITERS:
            pruned_counts.append(pruned_sum)
            moved = current + step_sizes[:, None] * gradient
            moved_norms = group_norms(moved)
            cutoff = step_sizes * penalty
            factor = jnp.maximum(moved_norms - cutoff, 0.0) / jnp.maximum(moved_norms, cutoff)
            current = (keep * factor)[:, None] * moved
    return (current, jnp.stack(correlations), jnp.stack(relative_gaps), jnp.stack(pruned_counts))


def local(design, targets, warm_start, active_mask, penalty_index):
    feat, samp = lax.axis_size("feat"), lax.axis_size("samp")
    rows, cols = design.shape
    fits = (
        feat == 2 * LINE
        and samp == 2 * CORES
        and rows % (2 * GROUP) == 0
        and rows // (2 * GROUP) >= 6
        and cols % (2 * CORES * LANES) == 0
        and targets.shape[1] == LANES
    )
    form = fused if fits else plain
    return form(design, targets, warm_start, active_mask, penalty_index)


def solution(mesh):
    placed = (P("samp", "feat"), P("samp", None), P("feat", None), P(None, "feat"), P())
    return jax.shard_map(
        local,
        mesh=mesh,
        in_specs=placed,
        out_specs=(P("feat", None), P(None, "feat"), P(), P()),
        check_vma=False,
    )
```

```python
import functools

import jax
import jax.numpy as jnp
from jax import lax
from jax.experimental import pallas as pl
from jax.experimental.pallas import tpu as pltpu
from jax.sharding import PartitionSpec as P

ITERS = 2
F32 = jnp.float32
BF16 = jnp.bfloat16
LANES = 128
GROUP = 256
PER = 4
SHIFT = 1
LINE = 4
CORES = 2
STATS = 16
MESH = pl.DeviceIdType.MESH


def fold(row, combine):
    pieces = [row[:, at : at + LANES] for at in range(0, row.shape[1], LANES)]
    return functools.reduce(combine, pieces)


def column_norms(matrix):
    return jnp.sqrt(jnp.sum(matrix * matrix, axis=0, keepdims=True))


def kernel(
    stored, stored_targets, stored_warm, stored_mask, stored_index, coef_out, corr_out, info_out,
    design, targets, warm, mask, index, half, cur, ysend, yrecv, zsend, frecv, erecv, resid, mine, turned,
    gacc, cacc, drecv, dcrecv, gsend, grecv, sqs, sqr, coefs, nrm, mx, sums, exf, exs,
    l_s, t_s, gv_r, tv_r, gv_s, tv_s, w_s, k_s, i_s, o_s, y_s, z_s, b_s, a_s, d_s, dc_s, x_s, h_s, q_s, c_s, n_s, m_s, ef_s, es_s,
    y_r, f_r, e_r, a_r, d_r, dc_r, h_r, x_r, m_r, q_r, c_r, n_r, ef_r, es_r,
):
    T = ITERS + 1
    F = exf.shape[0]
    S = exs.shape[0]
    R, C = stored.shape
    K = targets.shape[1]
    H = R // 2
    G = H // GROUP
    full = G + SHIFT
    b = GROUP // PER
    pieces = CORES * 2
    W = C // pieces
    f = lax.axis_index("feat")
    s = lax.axis_index("samp")
    z, y = f // 2, lax.rem(f, 2)
    x, c = s // CORES, lax.rem(s, CORES)
    mid = lax.rem((z + 1) // 2, 2)
    is_mid = mid == 1
    is_end = mid == 0
    takes = c == CORES - 1
    gives = c == 0
    held = G - SHIFT + SHIFT * c
    count = held + SHIFT * c
    me = f * CORES + c
    near = z + 1 - 2 * lax.rem(z, 2)
    across = {"feat": z * 2 + 1 - y}
    nearby = {"feat": near * 2 + y}
    middle = {"feat": (LINE - 1 - z) * 2 + y}
    sibling = {"samp": x * CORES + 1 - c}
    facing = {"samp": (1 - x) * CORES + c}

    def remote(src, dst, send, recv, to):
        return pltpu.make_async_remote_copy(
            src_ref=src, dst_ref=dst, send_sem=send, recv_sem=recv, device_id=to, device_id_type=MESH
        )

    def peer(off):
        to = lax.rem(me + off, F * CORES)
        return {"feat": to // CORES, "samp": x * CORES + lax.rem(to, CORES)}

    def rows_at(side, g):
        return pl.ds(pl.multiple_of((side * full + g) * GROUP, GROUP), GROUP)

    def stored_at(side, g):
        return pl.ds(pl.multiple_of(side * H + g * GROUP, GROUP), GROUP)

    def load(side, g):
        src, dst = stored.at[stored_at(side, g), :], design.at[rows_at(side, g), :]
        return pltpu.make_async_copy(src, dst, l_s.at[side, g])

    def give(side):
        src, dst = stored.at[stored_at(side, G - 1), :], design.at[rows_at(side, full - 1), :]
        return remote(src, dst, gv_s, gv_r.at[side], sibling)

    def load_targets(side):
        src, dst = stored_targets.at[side * H : (side + 1) * H, :], targets.at[side * full * GROUP : side * full * GROUP + H, :]
        return pltpu.make_async_copy(src, dst, t_s.at[side])

    def give_targets(side):
        src = stored_targets.at[stored_at(side, G - 1), :]
        return remote(src, targets.at[rows_at(side, full - 1), :], tv_s, tv_r.at[side], sibling)

    load_warm = pltpu.make_async_copy(stored_warm, warm, w_s)
    load_mask = pltpu.make_async_copy(stored_mask, mask, k_s)
    load_index = pltpu.make_async_copy(stored_index, index, i_s)
    store_coefs = pltpu.make_async_copy(coefs, coef_out, o_s)

    def copy_y(t, k):
        at = (t, k)
        return remote(ysend.at[at], yrecv.at[at], y_s, y_r.at[k], across)

    def copy_fold(t, k):
        at = (t, k)
        return remote(zsend.at[at], frecv.at[at], z_s, f_r.at[k], nearby)

    def copy_middle(t, k):
        at = (t, k)
        return remote(zsend.at[at], erecv.at[at], z_s, e_r.at[k], middle)

    def copy_out(t, k):
        ref = resid.at[t, y, k]
        return remote(ref, ref, b_s, f_r.at[k], nearby)

    def copy_a(t, k):
        ref = resid.at[t, y, k]
        return remote(ref, ref, a_s, a_r.at[k], across)

    def copy_d(t, j):
        at = (t, j)
        if t == T:
            return remote(cacc.at[(1 - c) * 2 + j], dcrecv.at[j], dc_s, dc_r.at[j], sibling)
        return remote(gacc.at[t, (1 - c) * 2 + j], drecv.at[at], d_s, d_r.at[j], sibling)

    def copy_x(t, j):
        at = (t, j)
        return remote(gsend.at[at], grecv.at[at], x_s, x_r.at[at], facing)

    def copy_h(t, j):
        ref = half.at[t, c * 2 + j]
        return remote(ref, ref, h_s, h_r.at[j], sibling)

    def copy_q():
        return remote(sqs, sqr, q_s, q_r, facing)

    def copy_c():
        ref = coefs.at[pl.ds(c * 2, 2)]
        return remote(ref, ref, c_s, c_r, sibling)

    def copy_n():
        return remote(nrm.at[c], nrm.at[c], n_s, n_r, sibling)

    def copy_m(t, off):
        ref = mx.at[t, me]
        return remote(ref, ref, m_s, m_r.at[t], peer(off))

    def copy_ef(off):
        to = {"feat": lax.rem(f + off, F)}
        return remote(exf.at[f], exf.at[f], ef_s, ef_r, to)

    def copy_es(off):
        to = {"samp": lax.rem(s + off, S)}
        return remote(exs.at[s], exs.at[s], es_s, es_r, to)

    others_f = exf.at[pl.ds(0, F - 1)]
    others_s = exs.at[pl.ds(0, S - 1)]

    def each(first, count, body):
        def step(at, carry):
            body(at)
            return carry

        lax.fori_loop(first, count, step, 0)

    load_warm.start()
    each(0, held, lambda g: load(1 - y, g).start())
    barrier = pltpu.get_barrier_semaphore()
    for off in range(1, F * CORES):
        pl.semaphore_signal(barrier, inc=1, device_id=peer(off), device_id_type=MESH)
    for core in range(CORES):
        to = {"samp": (1 - x) * CORES + core}
        pl.semaphore_signal(barrier, inc=1, device_id=to, device_id_type=MESH)
    each(0, held, lambda g: load(y, g).start())
    for side in range(2):
        load_targets(side).start()
    load_mask.start()
    load_index.start()

    def share(t, side, g):
        return jnp.dot(design[rows_at(side, g), :], half[t].reshape(C, K), preferred_element_type=F32)

    def products(acc, rows, chunk, order):
        turned[...] = chunk.T
        for p in order:
            cols = pl.ds(pl.multiple_of(p * W, W), W)
            piece = jnp.dot(turned[...], design[rows, cols], preferred_element_type=F32)
            acc[p, 0:K] = acc[p, 0:K] + piece

    def grad_group(t, side, g, order=tuple(range(pieces))):
        chunk = resid[t, side, pl.ds(g * PER, PER)].reshape(GROUP, K)
        products(gacc.at[t], rows_at(side, g), chunk, order)

    def corr_group(side, g):
        rows = rows_at(side, g)
        products(cacc, rows, targets[rows, :], range(pieces))
        tall = 16

        def body(i, acc):
            block = design[pl.ds(pl.multiple_of((side * full + g) * GROUP + i * tall, tall), tall), :].astype(F32)
            block = block * block
            return acc + block[:8] + block[8:]

        acc = lax.fori_loop(0, GROUP // tall, body, jnp.zeros((8, C), F32), unroll=4)
        for p in range(pieces):
            cacc[p, K : K + 8] = cacc[p, K : K + 8] + acc[:, p * W : (p + 1) * W]

    def send_group(t, g, ready=True):
        if t == 0:
            @pl.when(g < held)
            def _():
                load(1 - y, g).wait()

            @pl.when(g >= held)
            def _():
                give(1 - y).wait_recv()

        part = share(t, 1 - y, g).astype(BF16).reshape(PER, b, K)
        for j in range(PER):
            ysend[t, g * PER + j] = part[j]
        if not ready:
            pl.semaphore_wait(barrier, F * CORES + CORES - 1)
        for j in range(PER):
            copy_y(t, g * PER + j).start()

    def fold_group(t, g):
        mine[...] = share(t, y, g)
        for j in range(PER):
            k = g * PER + j
            own = mine[j * b : (j + 1) * b]
            copy_y(t, k).wait_recv()

            @pl.when(is_end)
            def _():
                zsend[t, k] = (own + yrecv[t, k].astype(F32)).astype(BF16)
                copy_fold(t, k).start()

            @pl.when(is_mid)
            def _():
                copy_fold(t, k).wait_recv()
                zsend[t, k] = (own + yrecv[t, k].astype(F32) + frecv[t, k].astype(F32)).astype(BF16)
                copy_middle(t, k).start()

    def resid_group(t, g):
        @pl.when(is_end)
        def _():
            for j in range(PER):
                copy_out(t, g * PER + j).wait_recv()
                copy_a(t, g * PER + j).start()

        @pl.when(is_mid)
        def _():
            rr = jnp.zeros((1, K), F32)
            ry = jnp.zeros((1, K), F32)
            for j in range(PER):
                k = g * PER + j
                at = pl.ds(pl.multiple_of(y * full * GROUP + k * b, b), b)
                goal = targets[at, :].astype(F32)
                copy_middle(t, k).wait_recv()
                fitted = zsend[t, k].astype(F32) + erecv[t, k].astype(F32)
                rounded = (goal - fitted).astype(BF16)
                resid[t, y, k] = rounded
                copy_a(t, k).start()
                copy_out(t, k).start()
                wide = rounded.astype(F32)
                rr = rr + jnp.sum(wide * wide, axis=0, keepdims=True)
                ry = ry + jnp.sum(wide * goal, axis=0, keepdims=True)
            sums[t : t + 1] = sums[t : t + 1] + 0.5 * rr
            sums[T + t : T + t + 1] = sums[T + t : T + t + 1] + 0.5 * ry

        grad_group(t, y, g)

    def last_group(t, g, final=False):
        for j in range(PER):
            copy_a(t, g * PER + j).wait_recv()
        if final:
            grad_group(t, 1 - y, g, ((1 - c) * 2, (1 - c) * 2 + 1))
            for j in range(2):
                copy_d(t, j).start()
            grad_group(t, 1 - y, g, (c * 2, c * 2 + 1))
        else:
            grad_group(t, 1 - y, g)

    lag_fold = 3 * mid
    lag_resid = jnp.where(is_mid, G - 2, count - 1)
    lag_last = lag_resid + 2 + mid
    steps = lag_last + count - 1

    def run(t, first, until):
        def step(at):
            to_fold = at - lag_fold
            to_resid = at - lag_resid
            to_last = at - lag_last

            @pl.when((to_fold >= 0) & (to_fold < count))
            def _():
                fold_group(t, to_fold)

            @pl.when((to_resid >= 0) & (to_resid < count))
            def _():
                resid_group(t, to_resid)

            @pl.when(to_last >= 0)
            def _():
                last_group(t, to_last)

            if t == 0:
                @pl.when(at < count)
                def _():
                    corr_group(0, at)
                    corr_group(1, at)

        each(first, until, step)

    def chip_sum(t, j):
        p = c * 2 + j
        copy_d(t, j).wait_recv()
        if t == T:
            both = cacc[p] + dcrecv[j]
            sqs[j] = both[K : K + 8]
            gsend[t, j] = both[:K].astype(BF16)
        else:
            gsend[t, j] = (gacc[t, p] + drecv[t, j]).astype(BF16)
        copy_x(t, j).start()

    def whole_sum(t, j):
        copy_x(t, j).wait_recv()
        return gsend[t, j].astype(F32) + grecv[t, j].astype(F32)

    def spread(t, rows):
        most = fold(jnp.concatenate(rows, axis=1), jnp.maximum)
        mx[t, me] = jnp.broadcast_to(most, (8, LANES))
        for off in range(1, F * CORES):
            copy_m(t, off).start()

    def highest(t):
        several = mx.at[t, pl.ds(0, F * CORES - 1)]
        remote(several, several, m_s, m_r.at[t], peer(1)).wait_recv()
        tile = functools.reduce(jnp.maximum, [mx[t, at] for at in range(F * CORES)])
        return jnp.max(tile[0:1], axis=1, keepdims=True)

    def add_row(at, row):
        sums[at : at + 1] = sums[at : at + 1] + 0.5 * row

    load_warm.wait()
    half[0] = warm[...].astype(BF16).reshape(pieces, W, K)
    send_group(0, 0, False)

    @pl.when(gives)
    def _():
        give(y).start()
        give(1 - y).start()
        for side in range(2):
            give_targets(side).start()

    each(1, count, lambda g: send_group(0, g))
    sums[...] = jnp.zeros_like(sums)
    cacc[...] = jnp.zeros_like(cacc)
    gacc[...] = jnp.zeros_like(gacc)
    for j in range(2):
        cur[j] = warm[pl.ds(pl.multiple_of((c * 2 + j) * W, W), W), :].T
        add_row(2 * T, fold(column_norms(cur[j]), jnp.add))
    nrm[c] = jnp.zeros((8, 2 * W), F32)
    each(0, held, lambda g: load(y, g).wait())
    for side in range(2):
        load_targets(side).wait()

    @pl.when(takes)
    def _():
        give(y).wait_recv()
        for side in range(2):
            give_targets(side).wait_recv()


    penalty = None
    step_sizes = None
    for t in range(T):
        if t > 0:
            each(0, count, lambda g: send_group(t, g))
        if t == 0:
            run(0, 0, count)
            for j in range(2):
                copy_d(T, j).start()
            run(0, count, count + 2)
            for j in range(2):
                chip_sum(T, j)
            copy_q().start()
            run(0, count + 2, count + 5)
            spread(T, [column_norms(whole_sum(T, j)) for j in range(2)])
            run(0, count + 5, steps)
        elif t == ITERS:
            run(t, 0, steps - 2)
            exf[f] = sums[...]
            for off in range(1, F):
                copy_ef(off).start()
            run(t, steps - 2, steps)
        else:
            run(t, 0, steps)
        last_group(t, count - 1, True)
        for j in range(2):
            chip_sum(t, j)
        if t == 0:
            load_mask.wait()
            load_index.wait()
            penalty = highest(T) / (8.0 + 4.0 * index[0].astype(F32))
            step_sizes = []
            copy_q().wait_recv()
            for j in range(2):
                squares = jnp.sum(sqs[j] + sqr[j], axis=0, keepdims=True)
                step_sizes.append(0.5 / (1.0 + squares))
        if t == ITERS:
            copy_c().wait_recv()
            store_coefs.start()
            remote(others_f, others_f, ef_s, ef_r, across).wait_recv()
            exs[s] = functools.reduce(jnp.add, [exf[at] for at in range(F)])
            for off in range(1, S):
                copy_es(off).start()
        norms = []
        for j in range(2):
            gradient = whole_sum(t, j)
            norms.append(column_norms(gradient))
            if t < ITERS:
                at = pl.ds(pl.multiple_of((c * 2 + j) * W, W), W)
                keep = mask[t : t + 1, at].astype(F32)
                moved = cur[j] + step_sizes[j] * gradient
                moved_norms = column_norms(moved)
                cutoff = step_sizes[j] * penalty
                factor = jnp.maximum(moved_norms - cutoff, 0.0) / jnp.maximum(moved_norms, cutoff)
                after = (keep * factor) * moved
                cur[j] = after
                upright = after.T
                half[t + 1, c * 2 + j] = upright.astype(BF16)
                copy_h(t + 1, j).start()
                if t + 1 == ITERS:
                    coefs[c * 2 + j] = upright
                add_row(3 * T + t, fold(1.0 - keep, jnp.add))
                add_row(2 * T + t + 1, fold(column_norms(after), jnp.add))
            nrm[c, t : t + 1, j * W : (j + 1) * W] = norms[j]
        spread(t, norms)
        if t + 1 == ITERS:
            copy_c().start()
        if t < ITERS:
            for j in range(2):
                copy_h(t + 1, j).wait_recv()

    copy_n().start()
    remote(others_s, others_s, es_s, es_r, sibling).wait_recv()
    merged = functools.reduce(jnp.add, [exs[at] for at in range(S)])
    added_up = jnp.sum(merged, axis=1, keepdims=True)
    copy_n().wait_recv()
    lines = []
    for t in range(T):
        rr, ry, bn = (added_up[at : at + 1] for at in (t, T + t, 2 * T + t))
        scale = jnp.maximum(penalty, highest(t))
        primal = 0.5 * rr + penalty * bn
        ratio = penalty / scale
        dual = ratio * ry - 0.5 * ratio * ratio * rr
        lines.append((primal - dual) / (primal + 1.0))
        for core in range(CORES):
            corr_out[t : t + 1, core * 2 * W : (core + 1) * 2 * W] = nrm[core, t : t + 1, :] / scale
    for t in range(ITERS):
        lines.append(added_up[3 * T + t : 3 * T + t + 1])
    for at, line in enumerate(lines):
        info_out[at : at + 1, :] = jnp.broadcast_to(line, (1, LANES))

    store_coefs.wait()

    def drain(ref, sem):
        remote(ref, ref, sem, n_r, sibling).wait_send()

    def drain_chunks(ref):
        drain(ref, y_s)
        drain(ref, z_s)
        drain(ref, a_s)

        @pl.when(is_mid)
        def _():
            drain(ref, b_s)

    @pl.when(takes)
    def _():
        drain_chunks(ysend)

    @pl.when(gives)
    def _():
        drain_chunks(ysend.at[:, pl.ds(0, (G - SHIFT) * PER)])
        drain(design.at[pl.ds(0, 2 * GROUP), :], gv_s)
        drain(targets.at[pl.ds(0, 2 * GROUP), :], tv_s)

    drain(gacc.at[:, pl.ds(0, 2)], d_s)
    drain(cacc.at[pl.ds(0, 2)], dc_s)
    drain(gsend, x_s)
    drain(half.at[pl.ds(0, ITERS), pl.ds(0, 2)], h_s)
    drain(sqs, q_s)
    drain(coefs.at[pl.ds(0, 2)], c_s)
    drain(nrm.at[0], n_s)
    drain(mx.at[:, pl.ds(0, F * CORES - 1)], m_s)
    drain(others_f, ef_s)
    drain(others_s, es_s)


def finish(coef, corr, info, coef_out, corr_out, gaps_out, pruned_out):
    coef_out[...] = coef[...].reshape(coef_out.shape)
    corr_out[...] = corr[...]
    for at in range(ITERS + 1):
        gaps_out[at] = info[at, 0]
    for at in range(ITERS):
        pruned_out[at] = info[ITERS + 1 + at, 0]


def fused(design, targets, warm_start, active_mask, penalty_index):
    F, S = lax.axis_size("feat"), lax.axis_size("samp")
    R, C = design.shape
    K = targets.shape[1]
    T = ITERS + 1
    G = R // 2 // GROUP
    full = G + SHIFT
    N = full * PER
    b = GROUP // PER
    pieces = CORES * 2
    W = C // pieces
    dma = pltpu.SemaphoreType.DMA
    vmem = pl.BlockSpec(memory_space=pltpu.VMEM)
    anywhere = pl.BlockSpec(memory_space=pl.ANY)
    smem = pl.BlockSpec(memory_space=pltpu.SMEM)
    chunks = pltpu.VMEM((T, N, b, K), BF16)
    coefficients, correlations, info = pl.pallas_call(
        kernel,
        out_shape=(
            jax.ShapeDtypeStruct((pieces, W, K), F32),
            jax.ShapeDtypeStruct((T, C), F32),
            jax.ShapeDtypeStruct((8, LANES), F32),
        ),
        in_specs=[anywhere] * 5,
        out_specs=(anywhere, vmem, vmem),
        scratch_shapes=[
            pltpu.VMEM((2 * full * GROUP, C), BF16),
            pltpu.VMEM((2 * full * GROUP, K), BF16),
            pltpu.VMEM((C, K), F32),
            pltpu.VMEM((ITERS, C), jnp.int32),
            pltpu.SMEM((1,), jnp.int32),
            pltpu.VMEM((T, pieces, W, K), BF16),
            pltpu.VMEM((2, K, W), F32),
            chunks,
            chunks,
            chunks,
            chunks,
            chunks,
            pltpu.VMEM((T, 2, N, b, K), BF16),
            pltpu.VMEM((GROUP, K), F32),
            pltpu.VMEM((K, GROUP), BF16),
            pltpu.VMEM((T, pieces, K, W), F32),
            pltpu.VMEM((pieces, K + 8, W), F32),
            pltpu.VMEM((T, 2, K, W), F32),
            pltpu.VMEM((2, K + 8, W), F32),
            pltpu.VMEM((T + 1, 2, K, W), BF16),
            pltpu.VMEM((T + 1, 2, K, W), BF16),
            pltpu.VMEM((2, 8, W), F32),
            pltpu.VMEM((2, 8, W), F32),
            pltpu.VMEM((pieces, W, K), F32),
            pltpu.VMEM((CORES, 8, 2 * W), F32),
            pltpu.VMEM((T + 1, F * CORES, 8, LANES), F32),
            pltpu.VMEM((STATS, LANES), F32),
            pltpu.VMEM((F, STATS, LANES), F32),
            pltpu.VMEM((S, STATS, LANES), F32),
        ]
        + [dma((2, G))]
        + [dma((2,))] * 3
        + [dma] * 20
        + [dma((N,))] * 4
        + [dma((2,))] * 3
        + [dma((T + 1, 2)), dma((T + 1,))]
        + [dma] * 5,
        compiler_params=pltpu.CompilerParams(
            collective_id=0, has_side_effects=True, vmem_limit_bytes=62 * 1024 * 1024
        ),
    )(design, targets, warm_start, active_mask, penalty_index)
    return pl.pallas_call(
        finish,
        out_shape=(
            jax.ShapeDtypeStruct((C, K), F32),
            jax.ShapeDtypeStruct((T, C), F32),
            jax.ShapeDtypeStruct((T,), F32),
            jax.ShapeDtypeStruct((ITERS,), F32),
        ),
        in_specs=[vmem, vmem, smem],
        out_specs=(vmem, vmem, smem, smem),
    )(coefficients, correlations, info)


def group_norms(matrix):
    return jnp.sqrt(jnp.sum(matrix * matrix, axis=1))


def transpose_product(design, right_side):
    return lax.dot_general(
        design, right_side, (((0,), (0,)), ((), ())), preferred_element_type=jnp.float32
    )


def plain(design, targets, warm_start, active_mask, penalty_index):
    row_count, col_count = design.shape
    feat_size = lax.axis_size("feat")
    feat_slot = lax.axis_index("feat")
    block_rows = row_count // feat_size
    samp_first = (lax.axis_index("samp") == 0).astype(jnp.float32)
    corr_local = transpose_product(design, targets)
    squares_local = jnp.sum(jnp.square(design.astype(jnp.float32)), axis=0)
    corr_y, column_squares = lax.psum((corr_local, squares_local), "samp")
    penalty_max = lax.pmax(jnp.max(group_norms(corr_y)), "feat")
    penalty = penalty_max / (8.0 + 4.0 * penalty_index[0].astype(jnp.float32))
    step_sizes = 0.5 / (1.0 + column_squares)
    current = warm_start
    correlations = []
    relative_gaps = []
    pruned_counts = []
    own_targets = lax.dynamic_slice_in_dim(targets, feat_slot * block_rows, block_rows, 0)
    for iteration in range(ITERS + 1):
        current_half = current.astype(jnp.bfloat16)
        fitted_part = jnp.dot(design, current_half, preferred_element_type=jnp.float32)
        fitted = lax.psum(fitted_part, "feat")
        residual_all = (targets.astype(jnp.float32) - fitted).astype(jnp.bfloat16)
        residual = lax.dynamic_slice_in_dim(residual_all, feat_slot * block_rows, block_rows, 0)
        grad_local = transpose_product(design, residual_all)
        resid_float = residual.astype(jnp.float32)
        rr_local = jnp.sum(resid_float * resid_float)
        ry_local = jnp.sum(resid_float * own_targets.astype(jnp.float32))
        bn_local = samp_first * jnp.sum(group_norms(current))
        if iteration < ITERS:
            keep = active_mask[iteration].astype(jnp.float32)
            pruned_local = samp_first * jnp.sum(1.0 - keep)
        else:
            pruned_local = jnp.zeros((), jnp.float32)
        gradient = lax.psum(grad_local, "samp")
        grad_norms = group_norms(gradient)
        local_max = jnp.max(grad_norms)
        grad_top = lax.pmax(local_max, "feat")
        rr_sum, ry_sum, bn_sum, pruned_sum = lax.psum(
            (rr_local, ry_local, bn_local, pruned_local), ("feat", "samp")
        )
        scale = jnp.maximum(penalty, grad_top)
        correlations.append(grad_norms / scale)
        primal = 0.5 * rr_sum + penalty * bn_sum
        ratio = penalty / scale
        dual = ratio * ry_sum - 0.5 * ratio * ratio * rr_sum
        relative_gaps.append((primal - dual) / (primal + 1.0))
        if iteration < ITERS:
            pruned_counts.append(pruned_sum)
            moved = current + step_sizes[:, None] * gradient
            moved_norms = group_norms(moved)
            cutoff = step_sizes * penalty
            factor = jnp.maximum(moved_norms - cutoff, 0.0) / jnp.maximum(moved_norms, cutoff)
            current = (keep * factor)[:, None] * moved
    return (current, jnp.stack(correlations), jnp.stack(relative_gaps), jnp.stack(pruned_counts))


def local(design, targets, warm_start, active_mask, penalty_index):
    feat, samp = lax.axis_size("feat"), lax.axis_size("samp")
    rows, cols = design.shape
    fits = (
        feat == 2 * LINE
        and samp == 2 * CORES
        and rows % (2 * GROUP) == 0
        and rows // (2 * GROUP) >= 6
        and cols % (2 * CORES * LANES) == 0
        and targets.shape[1] == LANES
    )
    form = fused if fits else plain
    return form(design, targets, warm_start, active_mask, penalty_index)


def solution(mesh):
    placed = (P("samp", "feat"), P("samp", None), P("feat", None), P(None, "feat"), P())
    return jax.shard_map(
        local,
        mesh=mesh,
        in_specs=placed,
        out_specs=(P("feat", None), P(None, "feat"), P(), P()),
        check_vma=False,
    )
```

```python
import functools

import jax
import jax.numpy as jnp
from jax import lax
from jax.experimental import pallas as pl
from jax.experimental.pallas import tpu as pltpu
from jax.sharding import PartitionSpec as P

ITERS = 2
F32 = jnp.float32
BF16 = jnp.bfloat16
LANES = 128
GROUP = 256
PER = 4
SHIFT = 1
MID_RESID = 9
MID_LAST = 16
END_RESID = 24
LEAD = 3
CORR_SUM = 3
END_LAST = 13
LINE = 4
CORES = 2
STATS = 16
MESH = pl.DeviceIdType.MESH


def fold(row, combine):
    pieces = [row[:, at : at + LANES] for at in range(0, row.shape[1], LANES)]
    return functools.reduce(combine, pieces)


def column_norms(matrix):
    return jnp.sqrt(jnp.sum(matrix * matrix, axis=0, keepdims=True))


def kernel(
    stored, stored_targets, stored_warm, stored_mask, stored_index, coef_out, corr_out, info_out,
    design, targets, warm, mask, index, half, cur, ysend, yrecv, zsend, frecv, erecv, resid, mine, turned,
    gacc, cacc, drecv, dcrecv, gsend, grecv, sqs, sqr, coefs, nrm, mx, sums, exf, exs,
    l_s, t_s, gv_r, tv_r, gv_s, tv_s, w_s, k_s, i_s, o_s, y_s, z_s, b_s, a_s, d_s, dc_s, x_s, h_s, q_s, c_s, n_s, m_s, ef_s, es_s,
    y_r, f_r, e_r, a_r, d_r, dc_r, h_r, x_r, m_r, q_r, c_r, n_r, ef_r, es_r,
):
    T = ITERS + 1
    F = exf.shape[0]
    S = exs.shape[0]
    R, C = stored.shape
    K = targets.shape[1]
    H = R // 2
    G = H // GROUP
    full = G + SHIFT
    b = GROUP // PER
    pieces = CORES * 2
    W = C // pieces
    f = lax.axis_index("feat")
    s = lax.axis_index("samp")
    z, y = f // 2, lax.rem(f, 2)
    x, c = s // CORES, lax.rem(s, CORES)
    mid = lax.rem((z + 1) // 2, 2)
    is_mid = mid == 1
    is_end = mid == 0
    takes = c == CORES - 1
    gives = c == 0
    held = G - SHIFT + SHIFT * c
    count = held + SHIFT * c
    me = f * CORES + c
    near = z + 1 - 2 * lax.rem(z, 2)
    across = {"feat": z * 2 + 1 - y}
    nearby = {"feat": near * 2 + y}
    middle = {"feat": (LINE - 1 - z) * 2 + y}
    sibling = {"samp": x * CORES + 1 - c}
    facing = {"samp": (1 - x) * CORES + c}

    def remote(src, dst, send, recv, to):
        return pltpu.make_async_remote_copy(
            src_ref=src, dst_ref=dst, send_sem=send, recv_sem=recv, device_id=to, device_id_type=MESH
        )

    def peer(off):
        to = lax.rem(me + off, F * CORES)
        return {"feat": to // CORES, "samp": x * CORES + lax.rem(to, CORES)}

    def rows_at(side, g):
        return pl.ds(pl.multiple_of((side * full + g) * GROUP, GROUP), GROUP)

    def stored_at(side, g):
        return pl.ds(pl.multiple_of(side * H + g * GROUP, GROUP), GROUP)

    def load(side, g):
        src, dst = stored.at[stored_at(side, g), :], design.at[rows_at(side, g), :]
        return pltpu.make_async_copy(src, dst, l_s.at[side, g])

    def give(side):
        src, dst = stored.at[stored_at(side, G - 1), :], design.at[rows_at(side, full - 1), :]
        return remote(src, dst, gv_s, gv_r.at[side], sibling)

    def load_targets(side):
        src, dst = stored_targets.at[side * H : (side + 1) * H, :], targets.at[side * full * GROUP : side * full * GROUP + H, :]
        return pltpu.make_async_copy(src, dst, t_s.at[side])

    def give_targets(side):
        src = stored_targets.at[stored_at(side, G - 1), :]
        return remote(src, targets.at[rows_at(side, full - 1), :], tv_s, tv_r.at[side], sibling)

    load_warm = pltpu.make_async_copy(stored_warm, warm, w_s)
    load_mask = pltpu.make_async_copy(stored_mask, mask, k_s)
    load_index = pltpu.make_async_copy(stored_index, index, i_s)
    store_coefs = pltpu.make_async_copy(coefs, coef_out, o_s)

    def copy_y(t, k):
        at = (t, k)
        return remote(ysend.at[at], yrecv.at[at], y_s, y_r.at[k], across)

    def copy_fold(t, k):
        at = (t, k)
        return remote(zsend.at[at], frecv.at[at], z_s, f_r.at[k], nearby)

    def copy_middle(t, k):
        at = (t, k)
        return remote(zsend.at[at], erecv.at[at], z_s, e_r.at[k], middle)

    def copy_out(t, k):
        ref = resid.at[t, y, k]
        return remote(ref, ref, b_s, f_r.at[k], nearby)

    def copy_a(t, k):
        ref = resid.at[t, y, k]
        return remote(ref, ref, a_s, a_r.at[k // PER], across)

    def copy_d(t, j):
        at = (t, j)
        if t == T:
            return remote(cacc.at[(1 - c) * 2 + j], dcrecv.at[j], dc_s, dc_r.at[j], sibling)
        return remote(gacc.at[t, (1 - c) * 2 + j], drecv.at[at], d_s, d_r.at[j], sibling)

    def copy_x(t, j):
        at = (t, j)
        return remote(gsend.at[at], grecv.at[at], x_s, x_r.at[at], facing)

    def copy_h(t, j):
        ref = half.at[t, c * 2 + j]
        return remote(ref, ref, h_s, h_r.at[j], sibling)

    def copy_q():
        return remote(sqs, sqr, q_s, q_r, facing)

    def copy_c():
        ref = coefs.at[pl.ds(c * 2, 2)]
        return remote(ref, ref, c_s, c_r, sibling)

    def copy_n():
        return remote(nrm.at[c], nrm.at[c], n_s, n_r, sibling)

    def copy_m(t, off):
        ref = mx.at[t, me]
        return remote(ref, ref, m_s, m_r.at[t], peer(off))

    def copy_ef(off):
        to = {"feat": lax.rem(f + off, F)}
        return remote(exf.at[f], exf.at[f], ef_s, ef_r, to)

    def copy_es(off):
        to = {"samp": lax.rem(s + off, S)}
        return remote(exs.at[s], exs.at[s], es_s, es_r, to)

    others_f = exf.at[pl.ds(0, F - 1)]
    others_s = exs.at[pl.ds(0, S - 1)]

    def each(first, count, body):
        def step(at, carry):
            body(at)
            return carry

        lax.fori_loop(first, count, step, 0)

    load_warm.start()
    each(0, held, lambda g: load(1 - y, g).start())
    barrier = pltpu.get_barrier_semaphore()
    for off in range(1, F * CORES):
        pl.semaphore_signal(barrier, inc=1, device_id=peer(off), device_id_type=MESH)
    for core in range(CORES):
        to = {"samp": (1 - x) * CORES + core}
        pl.semaphore_signal(barrier, inc=1, device_id=to, device_id_type=MESH)
    each(0, held, lambda g: load(y, g).start())
    for side in range(2):
        load_targets(side).start()
    load_mask.start()
    load_index.start()

    def share(t, side, g):
        return jnp.dot(design[rows_at(side, g), :], half[t].reshape(C, K), preferred_element_type=F32)

    def products(acc, rows, chunk, order):
        turned[...] = chunk.T
        for p in order:
            cols = pl.ds(pl.multiple_of(p * W, W), W)
            piece = jnp.dot(turned[...], design[rows, cols], preferred_element_type=F32)
            acc[p, 0:K] = acc[p, 0:K] + piece

    def grad_group(t, side, g, order=tuple(range(pieces))):
        chunk = resid[t, side, pl.ds(g * PER, PER)].reshape(GROUP, K)
        products(gacc.at[t], rows_at(side, g), chunk, order)

    def corr_group(side, g):
        rows = rows_at(side, g)
        products(cacc, rows, targets[rows, :], range(pieces))
        tall = 16

        def body(i, acc):
            block = design[pl.ds(pl.multiple_of((side * full + g) * GROUP + i * tall, tall), tall), :].astype(F32)
            block = block * block
            return acc + block[:8] + block[8:]

        acc = lax.fori_loop(0, GROUP // tall, body, jnp.zeros((8, C), F32), unroll=4)
        for p in range(pieces):
            cacc[p, K : K + 8] = cacc[p, K : K + 8] + acc[:, p * W : (p + 1) * W]

    def send_group(t, g, ready=True):
        if t == 0:
            @pl.when(g < held)
            def _():
                load(1 - y, g).wait()

            @pl.when(g >= held)
            def _():
                give(1 - y).wait_recv()

        part = share(t, 1 - y, g).astype(BF16).reshape(PER, b, K)
        for j in range(PER):
            ysend[t, g * PER + j] = part[j]
        if not ready:
            pl.semaphore_wait(barrier, F * CORES + CORES - 1)
        for j in range(PER):
            copy_y(t, g * PER + j).start()

    def fold_chunk(t, k):
        g, j = k // PER, lax.rem(k, PER)

        @pl.when(j == 0)
        def _():
            mine[...] = share(t, y, g)

        own = mine[pl.ds(pl.multiple_of(j * b, b), b)]
        copy_y(t, k).wait_recv()

        @pl.when(is_end)
        def _():
            zsend[t, k] = (own + yrecv[t, k].astype(F32)).astype(BF16)
            copy_fold(t, k).start()

        @pl.when(is_mid)
        def _():
            copy_fold(t, k).wait_recv()
            zsend[t, k] = (own + yrecv[t, k].astype(F32) + frecv[t, k].astype(F32)).astype(BF16)
            copy_middle(t, k).start()

    def resid_chunk(t, k):
        @pl.when(is_end)
        def _():
            copy_out(t, k).wait_recv()
            copy_a(t, k).start()

        @pl.when(is_mid)
        def _():
            at = pl.ds(pl.multiple_of(y * full * GROUP + k * b, b), b)
            goal = targets[at, :].astype(F32)
            copy_middle(t, k).wait_recv()
            fitted = zsend[t, k].astype(F32) + erecv[t, k].astype(F32)
            rounded = (goal - fitted).astype(BF16)
            resid[t, y, k] = rounded
            copy_a(t, k).start()
            copy_out(t, k).start()
            wide = rounded.astype(F32)
            rr = jnp.sum(wide * wide, axis=0, keepdims=True)
            ry = jnp.sum(wide * goal, axis=0, keepdims=True)
            sums[t : t + 1] = sums[t : t + 1] + 0.5 * rr
            sums[T + t : T + t + 1] = sums[T + t : T + t + 1] + 0.5 * ry

        @pl.when(lax.rem(k, PER) == PER - 1)
        def _():
            grad_group(t, y, k // PER)

    def last_group(t, g, final=False):
        several = resid.at[t, 1 - y, pl.ds(g * PER, PER)]
        remote(several, several, a_s, a_r.at[g], across).wait_recv()
        if final:
            grad_group(t, 1 - y, g, ((1 - c) * 2, (1 - c) * 2 + 1))
            for j in range(2):
                copy_d(t, j).start()
            grad_group(t, 1 - y, g, (c * 2, c * 2 + 1))
        else:
            grad_group(t, 1 - y, g)

    chunk_count = count * PER
    lag_resid = jnp.where(is_mid, MID_RESID - 2 * c, END_RESID - 4 * c)
    lag_last = lag_resid + jnp.where(is_mid, MID_LAST, END_LAST - 2 * c)

    def lead(t):
        return LEAD * PER * mid if t == 0 else 0

    def steps(t):
        return lead(t) + lag_last + chunk_count - PER

    def run(t, first, until):
        def step(at):
            to_fold = at - lead(t)
            to_resid = to_fold - lag_resid
            to_last = to_fold - lag_last

            @pl.when((to_fold >= 0) & (to_fold < chunk_count))
            def _():
                fold_chunk(t, to_fold)

            @pl.when((to_resid >= 0) & (to_resid < chunk_count))
            def _():
                resid_chunk(t, to_resid)

            @pl.when((to_last >= 0) & (lax.rem(to_last + PER, PER) == PER - 1))
            def _():
                last_group(t, to_last // PER)

            if t == 0:
                @pl.when((at < chunk_count) & (lax.rem(at, PER) == 0))
                def _():
                    corr_group(0, at // PER)
                    corr_group(1, at // PER)

        each(first, until, step)

    def chip_sum(t, j):
        p = c * 2 + j
        copy_d(t, j).wait_recv()
        if t == T:
            both = cacc[p] + dcrecv[j]
            sqs[j] = both[K : K + 8]
            gsend[t, j] = both[:K].astype(BF16)
        else:
            gsend[t, j] = (gacc[t, p] + drecv[t, j]).astype(BF16)
        copy_x(t, j).start()

    def whole_sum(t, j):
        copy_x(t, j).wait_recv()
        return gsend[t, j].astype(F32) + grecv[t, j].astype(F32)

    def spread(t, rows):
        most = fold(jnp.concatenate(rows, axis=1), jnp.maximum)
        mx[t, me] = jnp.broadcast_to(most, (8, LANES))
        for off in range(1, F * CORES):
            copy_m(t, off).start()

    def highest(t):
        several = mx.at[t, pl.ds(0, F * CORES - 1)]
        remote(several, several, m_s, m_r.at[t], peer(1)).wait_recv()
        tile = functools.reduce(jnp.maximum, [mx[t, at] for at in range(F * CORES)])
        return jnp.max(tile[0:1], axis=1, keepdims=True)

    def add_row(at, row):
        sums[at : at + 1] = sums[at : at + 1] + 0.5 * row

    load_warm.wait()
    half[0] = warm[...].astype(BF16).reshape(pieces, W, K)
    send_group(0, 0, False)

    @pl.when(gives)
    def _():
        give(y).start()
        give(1 - y).start()
        for side in range(2):
            give_targets(side).start()

    each(1, count, lambda g: send_group(0, g))
    sums[...] = jnp.zeros_like(sums)
    cacc[...] = jnp.zeros_like(cacc)
    gacc[...] = jnp.zeros_like(gacc)
    for j in range(2):
        cur[j] = warm[pl.ds(pl.multiple_of((c * 2 + j) * W, W), W), :].T
        add_row(2 * T, fold(column_norms(cur[j]), jnp.add))
    nrm[c] = jnp.zeros((8, 2 * W), F32)
    each(0, held, lambda g: load(y, g).wait())
    for side in range(2):
        load_targets(side).wait()

    @pl.when(takes)
    def _():
        give(y).wait_recv()
        for side in range(2):
            give_targets(side).wait_recv()


    penalty = None
    step_sizes = None
    for t in range(T):
        if t > 0:
            each(0, count, lambda g: send_group(t, g))
        if t == 0:
            second = lead(0) + chunk_count + CORR_SUM * PER
            third = steps(0)
            run(0, 0, chunk_count)
            for j in range(2):
                copy_d(T, j).start()
            run(0, chunk_count, second)
            for j in range(2):
                chip_sum(T, j)
            copy_q().start()
            run(0, second, third)
            spread(T, [column_norms(whole_sum(T, j)) for j in range(2)])
        elif t == ITERS:
            run(t, 0, steps(t) - 2 * PER)
            exf[f] = sums[...]
            for off in range(1, F):
                copy_ef(off).start()
            run(t, steps(t) - 2 * PER, steps(t))
        else:
            run(t, 0, steps(t))
        last_group(t, count - 1, True)
        for j in range(2):
            chip_sum(t, j)
        if t == 0:
            load_mask.wait()
            load_index.wait()
            penalty = highest(T) / (8.0 + 4.0 * index[0].astype(F32))
            step_sizes = []
            copy_q().wait_recv()
            for j in range(2):
                squares = jnp.sum(sqs[j] + sqr[j], axis=0, keepdims=True)
                step_sizes.append(0.5 / (1.0 + squares))
        if t == ITERS:
            copy_c().wait_recv()
            store_coefs.start()
            remote(others_f, others_f, ef_s, ef_r, across).wait_recv()
            exs[s] = functools.reduce(jnp.add, [exf[at] for at in range(F)])
            for off in range(1, S):
                copy_es(off).start()
        norms = []
        for j in range(2):
            gradient = whole_sum(t, j)
            norms.append(column_norms(gradient))
            if t < ITERS:
                at = pl.ds(pl.multiple_of((c * 2 + j) * W, W), W)
                keep = mask[t : t + 1, at].astype(F32)
                moved = cur[j] + step_sizes[j] * gradient
                moved_norms = column_norms(moved)
                cutoff = step_sizes[j] * penalty
                factor = jnp.maximum(moved_norms - cutoff, 0.0) / jnp.maximum(moved_norms, cutoff)
                after = (keep * factor) * moved
                cur[j] = after
                upright = after.T
                half[t + 1, c * 2 + j] = upright.astype(BF16)
                copy_h(t + 1, j).start()
                if t + 1 == ITERS:
                    coefs[c * 2 + j] = upright
                add_row(3 * T + t, fold(1.0 - keep, jnp.add))
                add_row(2 * T + t + 1, fold(column_norms(after), jnp.add))
            nrm[c, t : t + 1, j * W : (j + 1) * W] = norms[j]
        spread(t, norms)
        if t + 1 == ITERS:
            copy_c().start()
        if t < ITERS:
            for j in range(2):
                copy_h(t + 1, j).wait_recv()

    copy_n().start()
    remote(others_s, others_s, es_s, es_r, sibling).wait_recv()
    merged = functools.reduce(jnp.add, [exs[at] for at in range(S)])
    added_up = jnp.sum(merged, axis=1, keepdims=True)
    copy_n().wait_recv()
    lines = []
    for t in range(T):
        rr, ry, bn = (added_up[at : at + 1] for at in (t, T + t, 2 * T + t))
        scale = jnp.maximum(penalty, highest(t))
        primal = 0.5 * rr + penalty * bn
        ratio = penalty / scale
        dual = ratio * ry - 0.5 * ratio * ratio * rr
        lines.append((primal - dual) / (primal + 1.0))
        for core in range(CORES):
            corr_out[t : t + 1, core * 2 * W : (core + 1) * 2 * W] = nrm[core, t : t + 1, :] / scale
    for t in range(ITERS):
        lines.append(added_up[3 * T + t : 3 * T + t + 1])
    for at, line in enumerate(lines):
        info_out[at : at + 1, :] = jnp.broadcast_to(line, (1, LANES))

    store_coefs.wait()

    def drain(ref, sem):
        remote(ref, ref, sem, n_r, sibling).wait_send()

    def drain_chunks(ref):
        drain(ref, y_s)
        drain(ref, z_s)
        drain(ref, a_s)

        @pl.when(is_mid)
        def _():
            drain(ref, b_s)

    @pl.when(takes)
    def _():
        drain_chunks(ysend)

    @pl.when(gives)
    def _():
        drain_chunks(ysend.at[:, pl.ds(0, (G - SHIFT) * PER)])
        drain(design.at[pl.ds(0, 2 * GROUP), :], gv_s)
        drain(targets.at[pl.ds(0, 2 * GROUP), :], tv_s)

    drain(gacc.at[:, pl.ds(0, 2)], d_s)
    drain(cacc.at[pl.ds(0, 2)], dc_s)
    drain(gsend, x_s)
    drain(half.at[pl.ds(0, ITERS), pl.ds(0, 2)], h_s)
    drain(sqs, q_s)
    drain(coefs.at[pl.ds(0, 2)], c_s)
    drain(nrm.at[0], n_s)
    drain(mx.at[:, pl.ds(0, F * CORES - 1)], m_s)
    drain(others_f, ef_s)
    drain(others_s, es_s)


def finish(coef, corr, info, coef_out, corr_out, gaps_out, pruned_out):
    coef_out[...] = coef[...].reshape(coef_out.shape)
    corr_out[...] = corr[...]
    for at in range(ITERS + 1):
        gaps_out[at] = info[at, 0]
    for at in range(ITERS):
        pruned_out[at] = info[ITERS + 1 + at, 0]


def fused(design, targets, warm_start, active_mask, penalty_index):
    F, S = lax.axis_size("feat"), lax.axis_size("samp")
    R, C = design.shape
    K = targets.shape[1]
    T = ITERS + 1
    G = R // 2 // GROUP
    full = G + SHIFT
    N = full * PER
    b = GROUP // PER
    pieces = CORES * 2
    W = C // pieces
    dma = pltpu.SemaphoreType.DMA
    vmem = pl.BlockSpec(memory_space=pltpu.VMEM)
    anywhere = pl.BlockSpec(memory_space=pl.ANY)
    smem = pl.BlockSpec(memory_space=pltpu.SMEM)
    chunks = pltpu.VMEM((T, N, b, K), BF16)
    coefficients, correlations, info = pl.pallas_call(
        kernel,
        out_shape=(
            jax.ShapeDtypeStruct((pieces, W, K), F32),
            jax.ShapeDtypeStruct((T, C), F32),
            jax.ShapeDtypeStruct((8, LANES), F32),
        ),
        in_specs=[anywhere] * 5,
        out_specs=(anywhere, vmem, vmem),
        scratch_shapes=[
            pltpu.VMEM((2 * full * GROUP, C), BF16),
            pltpu.VMEM((2 * full * GROUP, K), BF16),
            pltpu.VMEM((C, K), F32),
            pltpu.VMEM((ITERS, C), jnp.int32),
            pltpu.SMEM((1,), jnp.int32),
            pltpu.VMEM((T, pieces, W, K), BF16),
            pltpu.VMEM((2, K, W), F32),
            chunks,
            chunks,
            chunks,
            chunks,
            chunks,
            pltpu.VMEM((T, 2, N, b, K), BF16),
            pltpu.VMEM((GROUP, K), F32),
            pltpu.VMEM((K, GROUP), BF16),
            pltpu.VMEM((T, pieces, K, W), F32),
            pltpu.VMEM((pieces, K + 8, W), F32),
            pltpu.VMEM((T, 2, K, W), F32),
            pltpu.VMEM((2, K + 8, W), F32),
            pltpu.VMEM((T + 1, 2, K, W), BF16),
            pltpu.VMEM((T + 1, 2, K, W), BF16),
            pltpu.VMEM((2, 8, W), F32),
            pltpu.VMEM((2, 8, W), F32),
            pltpu.VMEM((pieces, W, K), F32),
            pltpu.VMEM((CORES, 8, 2 * W), F32),
            pltpu.VMEM((T + 1, F * CORES, 8, LANES), F32),
            pltpu.VMEM((STATS, LANES), F32),
            pltpu.VMEM((F, STATS, LANES), F32),
            pltpu.VMEM((S, STATS, LANES), F32),
        ]
        + [dma((2, G))]
        + [dma((2,))] * 3
        + [dma] * 20
        + [dma((N,))] * 3
        + [dma((full,))]
        + [dma((2,))] * 3
        + [dma((T + 1, 2)), dma((T + 1,))]
        + [dma] * 5,
        compiler_params=pltpu.CompilerParams(
            collective_id=0, has_side_effects=True, vmem_limit_bytes=62 * 1024 * 1024
        ),
    )(design, targets, warm_start, active_mask, penalty_index)
    return pl.pallas_call(
        finish,
        out_shape=(
            jax.ShapeDtypeStruct((C, K), F32),
            jax.ShapeDtypeStruct((T, C), F32),
            jax.ShapeDtypeStruct((T,), F32),
            jax.ShapeDtypeStruct((ITERS,), F32),
        ),
        in_specs=[vmem, vmem, smem],
        out_specs=(vmem, vmem, smem, smem),
    )(coefficients, correlations, info)


def group_norms(matrix):
    return jnp.sqrt(jnp.sum(matrix * matrix, axis=1))


def transpose_product(design, right_side):
    return lax.dot_general(
        design, right_side, (((0,), (0,)), ((), ())), preferred_element_type=jnp.float32
    )


def plain(design, targets, warm_start, active_mask, penalty_index):
    row_count, col_count = design.shape
    feat_size = lax.axis_size("feat")
    feat_slot = lax.axis_index("feat")
    block_rows = row_count // feat_size
    samp_first = (lax.axis_index("samp") == 0).astype(jnp.float32)
    corr_local = transpose_product(design, targets)
    squares_local = jnp.sum(jnp.square(design.astype(jnp.float32)), axis=0)
    corr_y, column_squares = lax.psum((corr_local, squares_local), "samp")
    penalty_max = lax.pmax(jnp.max(group_norms(corr_y)), "feat")
    penalty = penalty_max / (8.0 + 4.0 * penalty_index[0].astype(jnp.float32))
    step_sizes = 0.5 / (1.0 + column_squares)
    current = warm_start
    correlations = []
    relative_gaps = []
    pruned_counts = []
    own_targets = lax.dynamic_slice_in_dim(targets, feat_slot * block_rows, block_rows, 0)
    for iteration in range(ITERS + 1):
        current_half = current.astype(jnp.bfloat16)
        fitted_part = jnp.dot(design, current_half, preferred_element_type=jnp.float32)
        fitted = lax.psum(fitted_part, "feat")
        residual_all = (targets.astype(jnp.float32) - fitted).astype(jnp.bfloat16)
        residual = lax.dynamic_slice_in_dim(residual_all, feat_slot * block_rows, block_rows, 0)
        grad_local = transpose_product(design, residual_all)
        resid_float = residual.astype(jnp.float32)
        rr_local = jnp.sum(resid_float * resid_float)
        ry_local = jnp.sum(resid_float * own_targets.astype(jnp.float32))
        bn_local = samp_first * jnp.sum(group_norms(current))
        if iteration < ITERS:
            keep = active_mask[iteration].astype(jnp.float32)
            pruned_local = samp_first * jnp.sum(1.0 - keep)
        else:
            pruned_local = jnp.zeros((), jnp.float32)
        gradient = lax.psum(grad_local, "samp")
        grad_norms = group_norms(gradient)
        local_max = jnp.max(grad_norms)
        grad_top = lax.pmax(local_max, "feat")
        rr_sum, ry_sum, bn_sum, pruned_sum = lax.psum(
            (rr_local, ry_local, bn_local, pruned_local), ("feat", "samp")
        )
        scale = jnp.maximum(penalty, grad_top)
        correlations.append(grad_norms / scale)
        primal = 0.5 * rr_sum + penalty * bn_sum
        ratio = penalty / scale
        dual = ratio * ry_sum - 0.5 * ratio * ratio * rr_sum
        relative_gaps.append((primal - dual) / (primal + 1.0))
        if iteration < ITERS:
            pruned_counts.append(pruned_sum)
            moved = current + step_sizes[:, None] * gradient
            moved_norms = group_norms(moved)
            cutoff = step_sizes * penalty
            factor = jnp.maximum(moved_norms - cutoff, 0.0) / jnp.maximum(moved_norms, cutoff)
            current = (keep * factor)[:, None] * moved
    return (current, jnp.stack(correlations), jnp.stack(relative_gaps), jnp.stack(pruned_counts))


def local(design, targets, warm_start, active_mask, penalty_index):
    feat, samp = lax.axis_size("feat"), lax.axis_size("samp")
    rows, cols = design.shape
    fits = (
        feat == 2 * LINE
        and samp == 2 * CORES
        and rows % (2 * GROUP) == 0
        and rows // (2 * GROUP) >= 6
        and cols % (2 * CORES * LANES) == 0
        and targets.shape[1] == LANES
    )
    form = fused if fits else plain
    return form(design, targets, warm_start, active_mask, penalty_index)


def solution(mesh):
    placed = (P("samp", "feat"), P("samp", None), P("feat", None), P(None, "feat"), P())
    return jax.shard_map(
        local,
        mesh=mesh,
        in_specs=placed,
        out_specs=(P("feat", None), P(None, "feat"), P(), P()),
        check_vma=False,
    )
```

```python
import functools

import jax
import jax.numpy as jnp
from jax import lax
from jax.experimental import pallas as pl
from jax.experimental.pallas import tpu as pltpu
from jax.sharding import PartitionSpec as P

ITERS = 2
F32 = jnp.float32
BF16 = jnp.bfloat16
LANES = 128
GROUP = 256
PER = 4
SHIFT = 1
MID_RESID = 9
MID_LAST = 16
END_RESID = 24
LEAD = 3
CORR_SUM = 3
END_LAST = 13
LINE = 4
CORES = 2
STATS = 16
MESH = pl.DeviceIdType.MESH


def fold(row, combine):
    pieces = [row[:, at : at + LANES] for at in range(0, row.shape[1], LANES)]
    return functools.reduce(combine, pieces)


def column_norms(matrix):
    return jnp.sqrt(jnp.sum(matrix * matrix, axis=0, keepdims=True))


def kernel(
    stored, stored_targets, stored_warm, stored_mask, stored_index, coef_out, corr_out, info_out,
    design, targets, warm, mask, index, half, cur, ysend, yrecv, zsend, frecv, erecv, resid, mine, turned,
    gacc, cacc, drecv, dcrecv, gsend, grecv, sqs, sqr, coefs, nrm, mx, sums, exf, exs,
    l_s, t_s, gv_r, tv_r, gv_s, tv_s, w_s, k_s, i_s, o_s, y_s, z_s, b_s, a_s, d_s, dc_s, x_s, h_s, q_s, c_s, n_s, m_s, ef_s, es_s,
    y_r, f_r, e_r, a_r, d_r, dc_r, h_r, x_r, m_r, q_r, c_r, n_r, ef_r, es_r,
):
    T = ITERS + 1
    F = exf.shape[0]
    S = exs.shape[0]
    R, C = stored.shape
    K = targets.shape[1]
    H = R // 2
    G = H // GROUP
    full = G + SHIFT
    b = GROUP // PER
    pieces = CORES * 2
    W = C // pieces
    f = lax.axis_index("feat")
    s = lax.axis_index("samp")
    z, y = f // 2, lax.rem(f, 2)
    x, c = s // CORES, lax.rem(s, CORES)
    mid = lax.rem((z + 1) // 2, 2)
    is_mid = mid == 1
    is_end = mid == 0
    takes = c == CORES - 1
    gives = c == 0
    held = G - SHIFT + SHIFT * c
    count = held + SHIFT * c
    me = f * CORES + c
    near = z + 1 - 2 * lax.rem(z, 2)
    across = {"feat": z * 2 + 1 - y}
    nearby = {"feat": near * 2 + y}
    middle = {"feat": (LINE - 1 - z) * 2 + y}
    sibling = {"samp": x * CORES + 1 - c}
    facing = {"samp": (1 - x) * CORES + c}

    def remote(src, dst, send, recv, to):
        return pltpu.make_async_remote_copy(
            src_ref=src, dst_ref=dst, send_sem=send, recv_sem=recv, device_id=to, device_id_type=MESH
        )

    def peer(off):
        to = lax.rem(me + off, F * CORES)
        return {"feat": to // CORES, "samp": x * CORES + lax.rem(to, CORES)}

    def rows_at(side, g):
        return pl.ds(pl.multiple_of((side * full + g) * GROUP, GROUP), GROUP)

    def stored_at(side, g):
        return pl.ds(pl.multiple_of(side * H + g * GROUP, GROUP), GROUP)

    def load(side, g):
        src, dst = stored.at[stored_at(side, g), :], design.at[rows_at(side, g), :]
        return pltpu.make_async_copy(src, dst, l_s.at[side, g])

    def give(side):
        src, dst = stored.at[stored_at(side, G - 1), :], design.at[rows_at(side, full - 1), :]
        return remote(src, dst, gv_s, gv_r.at[side], sibling)

    def load_targets(side):
        src, dst = stored_targets.at[side * H : (side + 1) * H, :], targets.at[side * full * GROUP : side * full * GROUP + H, :]
        return pltpu.make_async_copy(src, dst, t_s.at[side])

    def give_targets(side):
        src = stored_targets.at[stored_at(side, G - 1), :]
        return remote(src, targets.at[rows_at(side, full - 1), :], tv_s, tv_r.at[side], sibling)

    load_warm = pltpu.make_async_copy(stored_warm, warm, w_s)
    load_mask = pltpu.make_async_copy(stored_mask, mask, k_s)
    load_index = pltpu.make_async_copy(stored_index, index, i_s)
    store_coefs = pltpu.make_async_copy(coefs, coef_out, o_s)

    def copy_y(t, k):
        at = (t, k)
        return remote(ysend.at[at], yrecv.at[at], y_s, y_r.at[k], across)

    def copy_fold(t, k):
        at = (t, k)
        return remote(zsend.at[at], frecv.at[at], z_s, f_r.at[k], nearby)

    def copy_middle(t, k):
        at = (t, k)
        return remote(zsend.at[at], erecv.at[at], z_s, e_r.at[k], middle)

    def copy_out(t, k):
        ref = resid.at[t, y, k]
        return remote(ref, ref, b_s, f_r.at[k], nearby)

    def copy_a(t, k):
        ref = resid.at[t, y, k]
        return remote(ref, ref, a_s, a_r.at[k // PER], across)

    def copy_d(t, j):
        at = (t, j)
        if t == T:
            return remote(cacc.at[(1 - c) * 2 + j], dcrecv.at[j], dc_s, dc_r.at[j], sibling)
        return remote(gacc.at[t, (1 - c) * 2 + j], drecv.at[at], d_s, d_r.at[j], sibling)

    def copy_x(t, j):
        at = (t, j)
        return remote(gsend.at[at], grecv.at[at], x_s, x_r.at[at], facing)

    def copy_h(t, j):
        ref = half.at[t, c * 2 + j]
        return remote(ref, ref, h_s, h_r.at[j], sibling)

    def copy_q():
        return remote(sqs, sqr, q_s, q_r, facing)

    def copy_c():
        ref = coefs.at[pl.ds(c * 2, 2)]
        return remote(ref, ref, c_s, c_r, sibling)

    def copy_n():
        return remote(nrm.at[c], nrm.at[c], n_s, n_r, sibling)

    def copy_m(t, off):
        ref = mx.at[t, me]
        return remote(ref, ref, m_s, m_r.at[t], peer(off))

    def copy_ef(off):
        to = {"feat": lax.rem(f + off, F)}
        return remote(exf.at[f], exf.at[f], ef_s, ef_r, to)

    def copy_es(off):
        to = {"samp": lax.rem(s + off, S)}
        return remote(exs.at[s], exs.at[s], es_s, es_r, to)

    others_f = exf.at[pl.ds(0, F - 1)]
    others_s = exs.at[pl.ds(0, S - 1)]

    def each(first, count, body):
        def step(at, carry):
            body(at)
            return carry

        lax.fori_loop(first, count, step, 0)

    load_warm.start()
    each(0, held, lambda g: load(1 - y, g).start())
    barrier = pltpu.get_barrier_semaphore()
    for off in range(1, F * CORES):
        pl.semaphore_signal(barrier, inc=1, device_id=peer(off), device_id_type=MESH)
    for core in range(CORES):
        to = {"samp": (1 - x) * CORES + core}
        pl.semaphore_signal(barrier, inc=1, device_id=to, device_id_type=MESH)
    each(0, held, lambda g: load(y, g).start())
    for side in range(2):
        load_targets(side).start()
    load_mask.start()
    load_index.start()

    def share(t, side, g):
        return jnp.dot(design[rows_at(side, g), :], half[t].reshape(C, K), preferred_element_type=F32)

    def products(acc, rows, chunk, order):
        turned[...] = chunk.T
        for p in order:
            cols = pl.ds(pl.multiple_of(p * W, W), W)
            piece = jnp.dot(turned[...], design[rows, cols], preferred_element_type=F32)
            acc[p, 0:K] = acc[p, 0:K] + piece

    def grad_group(t, side, g, order=tuple(range(pieces))):
        chunk = resid[t, side, pl.ds(g * PER, PER)].reshape(GROUP, K)
        products(gacc.at[t], rows_at(side, g), chunk, order)

    def corr_group(side, g):
        rows = rows_at(side, g)
        products(cacc, rows, targets[rows, :], range(pieces))
        tall = 16

        def body(i, acc):
            block = design[pl.ds(pl.multiple_of((side * full + g) * GROUP + i * tall, tall), tall), :].astype(F32)
            block = block * block
            return acc + block[:8] + block[8:]

        acc = lax.fori_loop(0, GROUP // tall, body, jnp.zeros((8, C), F32), unroll=4)
        for p in range(pieces):
            cacc[p, K : K + 8] = cacc[p, K : K + 8] + acc[:, p * W : (p + 1) * W]

    def send_group(t, g, ready=True):
        if t == 0:
            @pl.when(g < held)
            def _():
                load(1 - y, g).wait()

            @pl.when(g >= held)
            def _():
                give(1 - y).wait_recv()

        part = share(t, 1 - y, g).astype(BF16).reshape(PER, b, K)
        for j in range(PER):
            ysend[t, g * PER + j] = part[j]
        if not ready:
            pl.semaphore_wait(barrier, F * CORES + CORES - 1)
        for j in range(PER):
            copy_y(t, g * PER + j).start()

    def fold_chunk(t, k):
        g, j = k // PER, lax.rem(k, PER)

        @pl.when(j == 0)
        def _():
            mine[...] = share(t, y, g)

        own = mine[pl.ds(pl.multiple_of(j * b, b), b)]
        copy_y(t, k).wait_recv()

        @pl.when(is_end)
        def _():
            zsend[t, k] = (own + yrecv[t, k].astype(F32)).astype(BF16)
            copy_fold(t, k).start()

        @pl.when(is_mid)
        def _():
            copy_fold(t, k).wait_recv()
            zsend[t, k] = (own + yrecv[t, k].astype(F32) + frecv[t, k].astype(F32)).astype(BF16)
            copy_middle(t, k).start()

    def resid_chunk(t, k):
        @pl.when(is_end)
        def _():
            copy_out(t, k).wait_recv()
            copy_a(t, k).start()

        @pl.when(is_mid)
        def _():
            at = pl.ds(pl.multiple_of(y * full * GROUP + k * b, b), b)
            goal = targets[at, :].astype(F32)
            copy_middle(t, k).wait_recv()
            fitted = zsend[t, k].astype(F32) + erecv[t, k].astype(F32)
            rounded = (goal - fitted).astype(BF16)
            resid[t, y, k] = rounded
            copy_out(t, k).start()
            copy_a(t, k).start()
            wide = rounded.astype(F32)
            rr = jnp.sum(wide * wide, axis=0, keepdims=True)
            ry = jnp.sum(wide * goal, axis=0, keepdims=True)
            sums[t : t + 1] = sums[t : t + 1] + 0.5 * rr
            sums[T + t : T + t + 1] = sums[T + t : T + t + 1] + 0.5 * ry

        @pl.when(lax.rem(k, PER) == PER - 1)
        def _():
            grad_group(t, y, k // PER)

    def last_group(t, g, final=False):
        several = resid.at[t, 1 - y, pl.ds(g * PER, PER)]
        remote(several, several, a_s, a_r.at[g], across).wait_recv()
        if final:
            grad_group(t, 1 - y, g, ((1 - c) * 2, (1 - c) * 2 + 1))
            for j in range(2):
                copy_d(t, j).start()
            grad_group(t, 1 - y, g, (c * 2, c * 2 + 1))
        else:
            grad_group(t, 1 - y, g)

    chunk_count = count * PER
    lag_resid = jnp.where(is_mid, MID_RESID - 2 * c, END_RESID - 4 * c)
    lag_last = lag_resid + jnp.where(is_mid, MID_LAST, END_LAST - 2 * c)

    def lead(t):
        return LEAD * PER * mid if t == 0 else 0

    def steps(t):
        return lead(t) + lag_last + chunk_count - PER

    def run(t, first, until):
        def step(at):
            to_fold = at - lead(t)
            to_resid = to_fold - lag_resid
            to_last = to_fold - lag_last

            @pl.when((to_fold >= 0) & (to_fold < chunk_count))
            def _():
                fold_chunk(t, to_fold)

            @pl.when((to_resid >= 0) & (to_resid < chunk_count))
            def _():
                resid_chunk(t, to_resid)

            @pl.when((to_last >= 0) & (lax.rem(to_last + PER, PER) == PER - 1))
            def _():
                last_group(t, to_last // PER)

            if t == 0:
                @pl.when((at < chunk_count) & (lax.rem(at, PER) == 0))
                def _():
                    corr_group(0, at // PER)
                    corr_group(1, at // PER)

        each(first, until, step)

    def chip_sum(t, j):
        p = c * 2 + j
        copy_d(t, j).wait_recv()
        if t == T:
            both = cacc[p] + dcrecv[j]
            sqs[j] = both[K : K + 8]
            gsend[t, j] = both[:K].astype(BF16)
        else:
            gsend[t, j] = (gacc[t, p] + drecv[t, j]).astype(BF16)
        copy_x(t, j).start()

    def whole_sum(t, j):
        copy_x(t, j).wait_recv()
        return gsend[t, j].astype(F32) + grecv[t, j].astype(F32)

    def spread(t, rows):
        most = fold(jnp.concatenate(rows, axis=1), jnp.maximum)
        mx[t, me] = jnp.broadcast_to(most, (8, LANES))
        for off in range(1, F * CORES):
            copy_m(t, off).start()

    def highest(t):
        several = mx.at[t, pl.ds(0, F * CORES - 1)]
        remote(several, several, m_s, m_r.at[t], peer(1)).wait_recv()
        tile = functools.reduce(jnp.maximum, [mx[t, at] for at in range(F * CORES)])
        return jnp.max(tile[0:1], axis=1, keepdims=True)

    def add_row(at, row):
        sums[at : at + 1] = sums[at : at + 1] + 0.5 * row

    load_warm.wait()
    half[0] = warm[...].astype(BF16).reshape(pieces, W, K)
    send_group(0, 0, False)

    @pl.when(gives)
    def _():
        give(y).start()
        give(1 - y).start()
        for side in range(2):
            give_targets(side).start()

    each(1, count, lambda g: send_group(0, g))
    sums[...] = jnp.zeros_like(sums)
    cacc[...] = jnp.zeros_like(cacc)
    gacc[...] = jnp.zeros_like(gacc)
    for j in range(2):
        cur[j] = warm[pl.ds(pl.multiple_of((c * 2 + j) * W, W), W), :].T
        add_row(2 * T, fold(column_norms(cur[j]), jnp.add))
    nrm[c] = jnp.zeros((8, 2 * W), F32)
    each(0, held, lambda g: load(y, g).wait())
    for side in range(2):
        load_targets(side).wait()

    @pl.when(takes)
    def _():
        give(y).wait_recv()
        for side in range(2):
            give_targets(side).wait_recv()


    penalty = None
    step_sizes = None
    for t in range(T):
        if t > 0:
            each(0, count, lambda g: send_group(t, g))
        if t == 0:
            second = lead(0) + chunk_count + CORR_SUM * PER
            third = steps(0)
            run(0, 0, chunk_count)
            for j in range(2):
                copy_d(T, j).start()
            run(0, chunk_count, second)
            for j in range(2):
                chip_sum(T, j)
            copy_q().start()
            run(0, second, third)
            spread(T, [column_norms(whole_sum(T, j)) for j in range(2)])
        elif t == ITERS:
            run(t, 0, steps(t) - 2 * PER)
            exf[f] = sums[...]
            for off in range(1, F):
                copy_ef(off).start()
            run(t, steps(t) - 2 * PER, steps(t))
        else:
            run(t, 0, steps(t))
        last_group(t, count - 1, True)
        for j in range(2):
            chip_sum(t, j)
        if t == 0:
            load_mask.wait()
            load_index.wait()
            penalty = highest(T) / (8.0 + 4.0 * index[0].astype(F32))
            step_sizes = []
            copy_q().wait_recv()
            for j in range(2):
                squares = jnp.sum(sqs[j] + sqr[j], axis=0, keepdims=True)
                step_sizes.append(0.5 / (1.0 + squares))
        if t == ITERS:
            copy_c().wait_recv()
            store_coefs.start()
            remote(others_f, others_f, ef_s, ef_r, across).wait_recv()
            exs[s] = functools.reduce(jnp.add, [exf[at] for at in range(F)])
            for off in range(1, S):
                copy_es(off).start()
        norms = []
        for j in range(2):
            gradient = whole_sum(t, j)
            norms.append(column_norms(gradient))
            if t < ITERS:
                at = pl.ds(pl.multiple_of((c * 2 + j) * W, W), W)
                keep = mask[t : t + 1, at].astype(F32)
                moved = cur[j] + step_sizes[j] * gradient
                moved_norms = column_norms(moved)
                cutoff = step_sizes[j] * penalty
                factor = jnp.maximum(moved_norms - cutoff, 0.0) / jnp.maximum(moved_norms, cutoff)
                after = (keep * factor) * moved
                cur[j] = after
                upright = after.T
                half[t + 1, c * 2 + j] = upright.astype(BF16)
                copy_h(t + 1, j).start()
                if t + 1 == ITERS:
                    coefs[c * 2 + j] = upright
                add_row(3 * T + t, fold(1.0 - keep, jnp.add))
                add_row(2 * T + t + 1, fold(column_norms(after), jnp.add))
            nrm[c, t : t + 1, j * W : (j + 1) * W] = norms[j]
        spread(t, norms)
        if t + 1 == ITERS:
            copy_c().start()
        if t < ITERS:
            for j in range(2):
                copy_h(t + 1, j).wait_recv()

    copy_n().start()
    remote(others_s, others_s, es_s, es_r, sibling).wait_recv()
    merged = functools.reduce(jnp.add, [exs[at] for at in range(S)])
    added_up = jnp.sum(merged, axis=1, keepdims=True)
    copy_n().wait_recv()
    store_coefs.wait()

    def drain(ref, sem):
        remote(ref, ref, sem, n_r, sibling).wait_send()

    def drain_chunks(ref):
        drain(ref, y_s)
        drain(ref, z_s)
        drain(ref, a_s)

        @pl.when(is_mid)
        def _():
            drain(ref, b_s)

    @pl.when(takes)
    def _():
        drain_chunks(ysend)

    @pl.when(gives)
    def _():
        drain_chunks(ysend.at[:, pl.ds(0, (G - SHIFT) * PER)])
        drain(design.at[pl.ds(0, 2 * GROUP), :], gv_s)
        drain(targets.at[pl.ds(0, 2 * GROUP), :], tv_s)

    drain(gacc.at[:, pl.ds(0, 2)], d_s)
    drain(cacc.at[pl.ds(0, 2)], dc_s)
    drain(gsend, x_s)
    drain(half.at[pl.ds(0, ITERS), pl.ds(0, 2)], h_s)
    drain(sqs, q_s)
    drain(coefs.at[pl.ds(0, 2)], c_s)
    drain(nrm.at[0], n_s)
    drain(mx.at[:, pl.ds(0, F * CORES - 1)], m_s)
    drain(others_f, ef_s)
    drain(others_s, es_s)

    lines = []
    for t in range(T):
        rr, ry, bn = (added_up[at : at + 1] for at in (t, T + t, 2 * T + t))
        scale = jnp.maximum(penalty, highest(t))
        primal = 0.5 * rr + penalty * bn
        ratio = penalty / scale
        dual = ratio * ry - 0.5 * ratio * ratio * rr
        lines.append((primal - dual) / (primal + 1.0))
        for core in range(CORES):
            corr_out[t : t + 1, core * 2 * W : (core + 1) * 2 * W] = nrm[core, t : t + 1, :] / scale
    for t in range(ITERS):
        lines.append(added_up[3 * T + t : 3 * T + t + 1])
    for at, line in enumerate(lines):
        info_out[at : at + 1, :] = jnp.broadcast_to(line, (1, LANES))


def finish(coef, corr, info, coef_out, corr_out, gaps_out, pruned_out):
    coef_out[...] = coef[...].reshape(coef_out.shape)
    corr_out[...] = corr[...]
    for at in range(ITERS + 1):
        gaps_out[at] = info[at, 0]
    for at in range(ITERS):
        pruned_out[at] = info[ITERS + 1 + at, 0]


def fused(design, targets, warm_start, active_mask, penalty_index):
    F, S = lax.axis_size("feat"), lax.axis_size("samp")
    R, C = design.shape
    K = targets.shape[1]
    T = ITERS + 1
    G = R // 2 // GROUP
    full = G + SHIFT
    N = full * PER
    b = GROUP // PER
    pieces = CORES * 2
    W = C // pieces
    dma = pltpu.SemaphoreType.DMA
    vmem = pl.BlockSpec(memory_space=pltpu.VMEM)
    anywhere = pl.BlockSpec(memory_space=pl.ANY)
    smem = pl.BlockSpec(memory_space=pltpu.SMEM)
    chunks = pltpu.VMEM((T, N, b, K), BF16)
    coefficients, correlations, info = pl.pallas_call(
        kernel,
        out_shape=(
            jax.ShapeDtypeStruct((pieces, W, K), F32),
            jax.ShapeDtypeStruct((T, C), F32),
            jax.ShapeDtypeStruct((8, LANES), F32),
        ),
        in_specs=[anywhere] * 5,
        out_specs=(anywhere, vmem, vmem),
        scratch_shapes=[
            pltpu.VMEM((2 * full * GROUP, C), BF16),
            pltpu.VMEM((2 * full * GROUP, K), BF16),
            pltpu.VMEM((C, K), F32),
            pltpu.VMEM((ITERS, C), jnp.int32),
            pltpu.SMEM((1,), jnp.int32),
            pltpu.VMEM((T, pieces, W, K), BF16),
            pltpu.VMEM((2, K, W), F32),
            chunks,
            chunks,
            chunks,
            chunks,
            chunks,
            pltpu.VMEM((T, 2, N, b, K), BF16),
            pltpu.VMEM((GROUP, K), F32),
            pltpu.VMEM((K, GROUP), BF16),
            pltpu.VMEM((T, pieces, K, W), F32),
            pltpu.VMEM((pieces, K + 8, W), F32),
            pltpu.VMEM((T, 2, K, W), F32),
            pltpu.VMEM((2, K + 8, W), F32),
            pltpu.VMEM((T + 1, 2, K, W), BF16),
            pltpu.VMEM((T + 1, 2, K, W), BF16),
            pltpu.VMEM((2, 8, W), F32),
            pltpu.VMEM((2, 8, W), F32),
            pltpu.VMEM((pieces, W, K), F32),
            pltpu.VMEM((CORES, 8, 2 * W), F32),
            pltpu.VMEM((T + 1, F * CORES, 8, LANES), F32),
            pltpu.VMEM((STATS, LANES), F32),
            pltpu.VMEM((F, STATS, LANES), F32),
            pltpu.VMEM((S, STATS, LANES), F32),
        ]
        + [dma((2, G))]
        + [dma((2,))] * 3
        + [dma] * 20
        + [dma((N,))] * 3
        + [dma((full,))]
        + [dma((2,))] * 3
        + [dma((T + 1, 2)), dma((T + 1,))]
        + [dma] * 5,
        compiler_params=pltpu.CompilerParams(
            collective_id=0, has_side_effects=True, vmem_limit_bytes=62 * 1024 * 1024
        ),
    )(design, targets, warm_start, active_mask, penalty_index)
    return pl.pallas_call(
        finish,
        out_shape=(
            jax.ShapeDtypeStruct((C, K), F32),
            jax.ShapeDtypeStruct((T, C), F32),
            jax.ShapeDtypeStruct((T,), F32),
            jax.ShapeDtypeStruct((ITERS,), F32),
        ),
        in_specs=[vmem, vmem, smem],
        out_specs=(vmem, vmem, smem, smem),
    )(coefficients, correlations, info)


def group_norms(matrix):
    return jnp.sqrt(jnp.sum(matrix * matrix, axis=1))


def transpose_product(design, right_side):
    return lax.dot_general(
        design, right_side, (((0,), (0,)), ((), ())), preferred_element_type=jnp.float32
    )


def plain(design, targets, warm_start, active_mask, penalty_index):
    row_count, col_count = design.shape
    feat_size = lax.axis_size("feat")
    feat_slot = lax.axis_index("feat")
    block_rows = row_count // feat_size
    samp_first = (lax.axis_index("samp") == 0).astype(jnp.float32)
    corr_local = transpose_product(design, targets)
    squares_local = jnp.sum(jnp.square(design.astype(jnp.float32)), axis=0)
    corr_y, column_squares = lax.psum((corr_local, squares_local), "samp")
    penalty_max = lax.pmax(jnp.max(group_norms(corr_y)), "feat")
    penalty = penalty_max / (8.0 + 4.0 * penalty_index[0].astype(jnp.float32))
    step_sizes = 0.5 / (1.0 + column_squares)
    current = warm_start
    correlations = []
    relative_gaps = []
    pruned_counts = []
    own_targets = lax.dynamic_slice_in_dim(targets, feat_slot * block_rows, block_rows, 0)
    for iteration in range(ITERS + 1):
        current_half = current.astype(jnp.bfloat16)
        fitted_part = jnp.dot(design, current_half, preferred_element_type=jnp.float32)
        fitted = lax.psum(fitted_part, "feat")
        residual_all = (targets.astype(jnp.float32) - fitted).astype(jnp.bfloat16)
        residual = lax.dynamic_slice_in_dim(residual_all, feat_slot * block_rows, block_rows, 0)
        grad_local = transpose_product(design, residual_all)
        resid_float = residual.astype(jnp.float32)
        rr_local = jnp.sum(resid_float * resid_float)
        ry_local = jnp.sum(resid_float * own_targets.astype(jnp.float32))
        bn_local = samp_first * jnp.sum(group_norms(current))
        if iteration < ITERS:
            keep = active_mask[iteration].astype(jnp.float32)
            pruned_local = samp_first * jnp.sum(1.0 - keep)
        else:
            pruned_local = jnp.zeros((), jnp.float32)
        gradient = lax.psum(grad_local, "samp")
        grad_norms = group_norms(gradient)
        local_max = jnp.max(grad_norms)
        grad_top = lax.pmax(local_max, "feat")
        rr_sum, ry_sum, bn_sum, pruned_sum = lax.psum(
            (rr_local, ry_local, bn_local, pruned_local), ("feat", "samp")
        )
        scale = jnp.maximum(penalty, grad_top)
        correlations.append(grad_norms / scale)
        primal = 0.5 * rr_sum + penalty * bn_sum
        ratio = penalty / scale
        dual = ratio * ry_sum - 0.5 * ratio * ratio * rr_sum
        relative_gaps.append((primal - dual) / (primal + 1.0))
        if iteration < ITERS:
            pruned_counts.append(pruned_sum)
            moved = current + step_sizes[:, None] * gradient
            moved_norms = group_norms(moved)
            cutoff = step_sizes * penalty
            factor = jnp.maximum(moved_norms - cutoff, 0.0) / jnp.maximum(moved_norms, cutoff)
            current = (keep * factor)[:, None] * moved
    return (current, jnp.stack(correlations), jnp.stack(relative_gaps), jnp.stack(pruned_counts))


def local(design, targets, warm_start, active_mask, penalty_index):
    feat, samp = lax.axis_size("feat"), lax.axis_size("samp")
    rows, cols = design.shape
    fits = (
        feat == 2 * LINE
        and samp == 2 * CORES
        and rows % (2 * GROUP) == 0
        and rows // (2 * GROUP) >= 6
        and cols % (2 * CORES * LANES) == 0
        and targets.shape[1] == LANES
    )
    form = fused if fits else plain
    return form(design, targets, warm_start, active_mask, penalty_index)


def solution(mesh):
    placed = (P("samp", "feat"), P("samp", None), P("feat", None), P(None, "feat"), P())
    return jax.shard_map(
        local,
        mesh=mesh,
        in_specs=placed,
        out_specs=(P("feat", None), P(None, "feat"), P(), P()),
        check_vma=False,
    )
```
